32 devices in a mesh: mem: 4 (over z), tx: 4 (over y, core), ty: 2 (over x).
Axes of the slice: x: 2, y: 2, z: 4, core: 2. Of those that a mesh axis runs over, the one named last changes fastest.
Arguments:
- alpha: float32 [32, 4, 64, 64], P('mem', None, 'tx', 'ty'), may hold values from -6 to 6
- filter_rate: float32 [64, 64], P('tx', 'ty'), may hold values from 0.1 to 0.24
- block_list: int32 [4, 2, 32], P('tx', 'ty'), may hold values from 0 to 63, as said below
- interp_weights: float32 [4, 2, 32, 64, 256], P('tx', 'ty'), may hold values from -0.75 to 0.75
- perturbations: bfloat16 [32, 4, 4, 256, 256], P('mem', None, None, ('tx', 'ty')), may hold values from -1.5 to 1.5
- obs_cells: int32 [4, 2, 512], P('tx', 'ty'), may hold values from 0 to 8191
- obs_count: int32 [4, 2], P('tx', 'ty'), may hold values from 1 to 512, as said below
- departures: float32 [4, 2, 16, 512], P('tx', 'ty', 'mem'), may hold values from -6 to 6
- obs_weight: float32 [4, 2, 16, 512], P('tx', 'ty', 'mem'), may hold values from 0.25 to 2.5
Outputs:
- increment: float32 [16, 256, 256], P('mem', ('tx', 'ty'))
- weighted_departure: float32 [4, 2, 16, 512], P('tx', 'ty', 'mem')
- gradient: float32 [32, 4, 64, 64], P('mem', None, 'tx', 'ty')
The draws below stay inside these ranges and needn't reach their ends.
Inputs may be any that keep to these rules, and one draw needn't show every extreme that they name: `block_list`: entries name coarse blocks numbered as in the reference program, of any tile. Among the fine blocks of one tile, at most 2 distinct coarse blocks of any one tile are named; every tile names exactly 2 distinct blocks of its own. `obs_count`: some tile has all 512 slots in use in every draw.
All inputs are finite; a program needn't handle non-finite values.
Results may differ from the reference program's by a relative error of at most 0.0003.
Values sent between devices are 32-bit elements; how exact they have to be, the bound alone decides.
No kernel may reach another device: no remote copies, remote signals or barrier semaphores. Data moves between devices by JAX's collectives and lax.ppermute only.
A program may use at most 64 MiB of HBM per device.

```python
import math
import jax
import jax.numpy as jnp
from jax import lax

LEV = 4
VARS = 4
CB = 8
CXC = 16
CYC = 32
SWEEPS = 4
CAP = 2
OBS = 512
MEMBERS = 32
TILES_X = 4
TILES_Y = 2
NCX = 64
NCY = 64
SLABS = 16
BLK_DEV = 8
FBLK_DEV = 32
BCELLS = 256
CELLS_DEV = 8192
FBLOCKS = 256
N_TX = 4
N_TY = 2


def draw_block_list(key, part):
    tile_count = TILES_X * TILES_Y
    score_key = jax.random.fold_in(key, 101)
    step_key = jax.random.fold_in(key, 102)
    column_key = jax.random.fold_in(key, 105)
    slot_key = jax.random.fold_in(key, 103)
    full_key = jax.random.fold_in(key, 104)
    scores = jax.random.randint(score_key, (tile_count, tile_count, BLK_DEV), 0, 1 << 20) * BLK_DEV + jnp.arange(BLK_DEV, dtype=jnp.int32)
    chosen = jnp.argsort(scores, axis=-1)[:, :, :CAP].astype(jnp.int32)
    tile_ids = jnp.arange(tile_count, dtype=jnp.int32)[:, None]
    fine_ids = jnp.arange(FBLK_DEV, dtype=jnp.int32)[None, :]
    row_of = tile_ids // TILES_Y
    steps_x = jax.random.randint(step_key, (tile_count, FBLK_DEV), -1, 2)
    columns = jax.random.randint(column_key, (tile_count, FBLK_DEV), 0, TILES_Y)
    owner_rows = jnp.clip(row_of + steps_x, 0, TILES_X - 1)
    owners = owner_rows * TILES_Y + columns
    slot_ids = jax.random.randint(slot_key, (tile_count, FBLK_DEV), 0, CAP)
    own_first = fine_ids < CAP
    owners = jnp.where(own_first, tile_ids, owners)
    slot_ids = jnp.where(own_first, fine_ids, slot_ids)
    full_tile = jax.random.randint(full_key, (), 0, tile_count)
    near_count = 3 * TILES_Y
    spread = (tile_ids == full_tile) & (fine_ids >= CAP) & (fine_ids < CAP + near_count * CAP)
    near_index = (fine_ids - CAP) // CAP
    near_rows = jnp.clip(row_of + near_index // TILES_Y - 1, 0, TILES_X - 1)
    near_owner = near_rows * TILES_Y + near_index % TILES_Y
    owners = jnp.where(spread, near_owner, owners)
    slot_ids = jnp.where(spread, (fine_ids - CAP) % CAP, slot_ids)
    far_start = CAP + near_count * CAP
    far_spread = (tile_ids == full_tile) & (fine_ids >= far_start) & (fine_ids < far_start + CAP)
    far_owner = (full_tile + tile_count // 2) % tile_count
    owners = jnp.where(far_spread, far_owner, owners)
    slot_ids = jnp.where(far_spread, fine_ids - far_start, slot_ids)
    local_ids = chosen[jnp.broadcast_to(tile_ids, owners.shape), owners, slot_ids]
    return (owners * BLK_DEV + local_ids).reshape(TILES_X, TILES_Y, FBLK_DEV).astype(jnp.int32)


def draw_obs_count(key, part):
    shift_key = jax.random.fold_in(key, 201)
    jitter_key = jax.random.fold_in(key, 202)
    full_key = jax.random.fold_in(key, 203)
    shifts = jax.random.randint(shift_key, (TILES_X, TILES_Y), 0, 4)
    ceilings = OBS // jnp.left_shift(jnp.ones_like(shifts), shifts)
    jitter = jax.random.randint(jitter_key, (TILES_X, TILES_Y), 0, jnp.maximum(ceilings // 2, 1))
    counts = jnp.maximum(ceilings - jitter, 1)
    full_tile = jax.random.randint(full_key, (), 0, TILES_X * TILES_Y)
    flat_ids = jnp.arange(TILES_X * TILES_Y, dtype=jnp.int32).reshape(TILES_X, TILES_Y)
    return jnp.where(flat_ids == full_tile, OBS, counts).astype(jnp.int32)


def set_ends(values, own_key, low, high):
    longest = values.shape.index(max(values.shape))
    spots = []
    for shift in (0, 1):
        where = [jax.random.randint(jax.random.fold_in(own_key, axis), (), 0, length) for axis, length in enumerate(values.shape)]
        where[longest] = (where[longest] + shift) % values.shape[longest]
        spots.append(tuple(where))
    return values.at[spots[0]].set(low).at[spots[1]].set(high)


def block_levels(rng, dims, cuts, least, top_value):
    loudness, own = 1.0, jax.random.fold_in(rng, 6)
    for axis_at, parts in cuts:
        draws = jnp.exp(jax.random.uniform(jax.random.fold_in(own, axis_at), (parts,), jnp.float32, least / len(cuts), top_value / len(cuts)))
        loudness = loudness * jnp.repeat(draws, dims[axis_at] // parts).reshape([-1 if axis == axis_at else 1 for axis in range(len(dims))])
    return loudness


def noise(rng, shape, scale, limit, split=(), kind=jnp.bfloat16):
    entries = scale * jax.random.normal(rng, shape, jnp.float32)
    if split:
        entries = entries * block_levels(rng, shape, split, -0.22, 0.18)
    return jnp.clip(entries, -limit, limit).astype(kind)


def setup_inputs(seed: int = 0) -> dict:
    keys = jax.random.split(jax.random.key(seed), 10)
    alpha = noise(keys[0], (MEMBERS, LEV, NCX, NCY), 1.0, 6.0, ((0, 4), (2, 4), (3, 2)), jnp.float32)
    filter_rate = jnp.clip(0.1 + 0.13999999 * jax.random.uniform(keys[1], (NCX, NCY), jnp.float32) ** block_levels(keys[1], (NCX, NCY), ((0, 4), (1, 2)), -0.2, 0.2), 0.1, 0.24)
    block_list = draw_block_list(jax.random.fold_in(keys[9], 71), 0)
    interp_weights = noise(keys[3], (TILES_X, TILES_Y, FBLK_DEV, CB * CB, BCELLS), (CB * CB) ** -0.5, 0.75, ((0, 4), (1, 2)), jnp.float32)
    perturbations = noise(keys[4], (MEMBERS, LEV, VARS, FBLOCKS, BCELLS), 0.25, 1.5, ((0, 4), (3, 8)))
    obs_cells = set_ends(jax.random.randint(keys[5], (TILES_X, TILES_Y, OBS), 0, CELLS_DEV), jax.random.fold_in(keys[5], 1), 0, CELLS_DEV - 1).astype(jnp.int32)
    obs_count = draw_obs_count(jax.random.fold_in(keys[9], 71), 0)
    departures = noise(keys[7], (TILES_X, TILES_Y, SLABS, OBS), 1.0, 6.0, ((0, 4), (1, 2), (2, 4)), jnp.float32)
    obs_weight = jnp.clip(jnp.exp(math.log(2.5) - 2.3025851 * jax.random.uniform(keys[8], (TILES_X, TILES_Y, SLABS, OBS), jnp.float32) ** block_levels(keys[8], (TILES_X, TILES_Y, SLABS, OBS), ((0, 4), (1, 2), (2, 4)), -0.2, 0.2)), 0.25, 2.5)
    return {"alpha": alpha, "filter_rate": filter_rate, "block_list": block_list, "interp_weights": interp_weights, "perturbations": perturbations, "obs_cells": obs_cells, "obs_count": obs_count, "departures": departures, "obs_weight": obs_weight}


exact_mode = lax.Precision.HIGHEST


def beside_sum(coarse):
    padded = jnp.pad(coarse, ((0, 0), (1, 1), (1, 1)))
    return padded[:, 2:, 1:-1] + padded[:, :-2, 1:-1] + padded[:, 1:-1, 2:] + padded[:, 1:-1, :-2]


def smooth(coarse, filter_coef):
    for sweep_no in range(SWEEPS):
        coarse = coarse + filter_coef * (beside_sum(coarse) - 4.0 * coarse)
    return coarse


def smooth_adjoint(coarse, filter_coef):
    for sweep_no in range(SWEEPS):
        scaled = filter_coef * coarse
        coarse = coarse + beside_sum(scaled) - 4.0 * scaled
    return coarse


def to_blocks(coarse):
    row_count = coarse.shape[0]
    arranged = coarse.reshape(row_count, N_TX, CXC // CB, CB, N_TY, CYC // CB, CB).transpose(1, 4, 2, 5, 0, 3, 6)
    return arranged.reshape(-1, row_count, CB * CB)


def from_blocks(blocks, row_count):
    arranged = blocks.reshape(N_TX, N_TY, CXC // CB, CYC // CB, row_count, CB, CB).transpose(4, 0, 2, 5, 1, 3, 6)
    return arranged.reshape(row_count, NCX, NCY)


def reference(alpha, filter_rate, block_list, interp_weights, perturbations, obs_cells, obs_count, departures, obs_weight):
    row_count = MEMBERS * LEV
    tile_count = N_TX * N_TY
    filter_coef = filter_rate[None]
    smoothed = smooth(alpha.reshape(row_count, NCX, NCY), filter_coef)
    blocks = to_blocks(smoothed)
    wanted = block_list.reshape(-1).astype(jnp.int32)
    weights = interp_weights.reshape(-1, CB * CB, BCELLS)
    fine_alpha = jnp.einsum("frk,fkc->rfc", blocks[wanted], weights, precision=exact_mode)
    fine_alpha = fine_alpha.reshape(MEMBERS, LEV, -1, BCELLS)
    pert_full = perturbations.astype(jnp.float32)
    increment = jnp.sum(fine_alpha[:, :, None] * pert_full, axis=0).reshape(SLABS, -1, BCELLS)
    flat_inc = increment.reshape(SLABS, tile_count, CELLS_DEV)
    obs_where = obs_cells.reshape(tile_count, OBS).astype(jnp.int32)
    observed = jnp.take_along_axis(flat_inc, obs_where[None], axis=2).transpose(1, 0, 2)
    in_use = jnp.arange(OBS, dtype=jnp.int32)[None, None, :] < obs_count.reshape(tile_count, 1, 1)
    weighted = jnp.where(in_use, obs_weight.reshape(tile_count, SLABS, OBS) * (observed - departures.reshape(tile_count, SLABS, OBS)), 0.0)
    tile_ids = jnp.arange(tile_count, dtype=jnp.int32)[:, None, None]
    slab_ids = jnp.arange(SLABS, dtype=jnp.int32)[None, :, None]
    forcing = jnp.zeros((tile_count, SLABS, CELLS_DEV), jnp.float32).at[tile_ids, slab_ids, obs_where[:, None, :]].add(weighted)
    forcing = forcing.transpose(1, 0, 2).reshape(LEV, VARS, -1, BCELLS)
    fine_gradient = jnp.sum(pert_full * forcing[None], axis=2)
    contrib = jnp.einsum("rfc,fkc->frk", fine_gradient.reshape(row_count, -1, BCELLS), weights, precision=exact_mode)
    summed = jnp.zeros_like(blocks).at[wanted].add(contrib)
    adjoint = smooth_adjoint(from_blocks(summed, row_count), filter_coef)
    gradient = alpha + adjoint.reshape(alpha.shape)
    return increment, weighted.reshape(N_TX, N_TY, SLABS, OBS), gradient
```

```python
import functools

import jax
import jax.numpy as jnp
from jax import lax
from jax.experimental import pallas as pl
from jax.experimental.pallas import tpu as pltpu
from jax.sharding import PartitionSpec as P

CB = 8
SWEEPS = 4
LANES = 128
SUB = 8
PITCH_PAD = 8


VM = pl.BlockSpec(memory_space=pltpu.VMEM)
SM = pl.BlockSpec(memory_space=pltpu.SMEM)


def params(mib):
    return pltpu.CompilerParams(vmem_limit_bytes=mib << 20)


def split2(v, n):
    if n & (n - 1) == 0:
        return v >> (n.bit_length() - 1), v & (n - 1)
    return lax.div(v, n), lax.rem(v, n)


def hi_lo(v):
    hi = v.astype(jnp.bfloat16)
    return hi, (v - hi.astype(jnp.float32)).astype(jnp.bfloat16)


def lane_ids(shape):
    return lax.broadcasted_iota(jnp.int32, shape, len(shape) - 1)


class Sizes:
    def __init__(self, alpha, weights, perts, cells, departures):
        self.n_tx, self.n_ty, self.n_mem = (lax.axis_size(a) for a in ("tx", "ty", "mem"))
        self.tiles = self.n_tx * self.n_ty
        self.chips = self.tiles // 2
        self.members, self.levels, self.cx, self.cy = alpha.shape
        self.rows = self.members * self.levels
        self.rg = self.rows // SUB
        self.fine, self.block, self.bcells = weights.shape[2:]
        self.vars = perts.shape[2]
        self.slabs = self.levels * self.vars
        self.slab_dev = departures.shape[2]
        self.obs = cells.shape[-1]
        self.nx, self.ny = self.n_tx * self.cx, self.n_ty * self.cy
        self.groups = LANES // self.ny
        self.xl = self.nx // self.groups
        self.nq = LANES // self.cy
        self.xq = self.cx // self.nq
        self.t_rows = self.xq * self.rg
        self.ct = self.bcells // LANES
        self.ot = self.obs // LANES
        self.blk_x, self.blk_y = self.cx // CB, self.cy // CB
        assert self.n_tx % 2 == 0 and self.groups * self.ny == LANES and self.ny == CB * CB
        assert self.xl % CB == 0 and self.nq * self.cy == LANES and self.xq * self.nq == self.cx
        assert self.xq <= SUB and self.rows % SUB == 0 and self.groups == 2
        assert self.slab_dev * self.ot <= self.slabs

    def block_place(self, bid):
        tile, kb = split2(bid, self.blk_x * self.blk_y)
        a, b = split2(tile, self.n_ty)
        bx, by = split2(kb, self.blk_y)
        gx, gy = a * self.blk_x + bx, b * self.blk_y + by
        g, xg = split2(gx, self.xl // CB)
        return xg * CB + gy, g

    def tile_at(self, step, back, other_core):
        tx, ty = lax.axis_index("tx"), lax.axis_index("ty")
        half = self.n_tx // 2
        chip_y, core = split2(tx, 2)
        dy, dx = divmod(step, self.n_ty)
        if back:
            dy, dx = half - dy, self.n_ty - dx
        y = lax.rem(chip_y + dy, half)
        x = lax.rem(ty + dx, self.n_ty)
        if other_core:
            core = 1 - core
        return (y * 2 + core) * self.n_ty + x

    def chip_perm(self, step):
        half = self.n_tx // 2
        dy, dx = divmod(step, self.n_ty)
        pairs = []
        for y in range(half):
            for core in range(2):
                for x in range(self.n_ty):
                    to = ((y + dy) % half * 2 + core) * self.n_ty + (x + dx) % self.n_ty
                    pairs.append(((y * 2 + core) * self.n_ty + x, to))
        return pairs

    def core_perm(self):
        return [(i, (i // self.n_ty ^ 1) * self.n_ty + i % self.n_ty) for i in range(self.tiles)]

    def pieces(self):
        table = [[] for _ in range(self.xl)]
        for a in range(self.n_tx):
            for x in range(self.cx):
                g, xl = divmod(a * self.cx + x, self.xl)
                q, xq = divmod(x, self.xq)
                for b in range(self.n_ty):
                    table[xl].append((a * self.n_ty + b, xq, q, g * self.ny // self.cy + b))
        return table


def rolled(v, shift):
    shift %= LANES
    return v if shift == 0 else pltpu.roll(v, shift, v.ndim - 1)


def pack_kernel(z, alpha_ref, rate_ref, out_ref):
    out_ref[z.t_rows] = jnp.zeros((SUB, LANES), jnp.float32)
    for x in range(z.cx):
        q, xq = divmod(x, z.xq)
        lanes = slice(q * z.cy, (q + 1) * z.cy)
        v = alpha_ref[:, x, :]
        out_ref[xq * z.rg : (xq + 1) * z.rg, :, lanes] = v.reshape(z.rg, SUB, z.cy)
        out_ref[z.t_rows, xq : xq + 1, lanes] = rate_ref[x : x + 1, :]


def prep_kernel(z, weights_ref, cells_ref, stacked_ref, column_ref):
    k = z.block

    def one(f, carry):
        hi, lo = hi_lo(weights_ref[f])
        stacked_ref[f, 0:k, :] = hi
        stacked_ref[f, k : 2 * k, :] = hi
        stacked_ref[f, 2 * k : 3 * k, :] = lo
        return carry

    lax.fori_loop(0, z.fine, one, 0, unroll=2)
    _, col = split2(cells_ref[...], z.bcells)
    ids = lax.broadcasted_iota(jnp.int32, (z.bcells, z.obs), 0)
    column_ref[...] = jnp.where(ids == col, 1.0, 0.0).astype(jnp.bfloat16)


def fill_edges(z, ref):
    lane = lane_ids((z.rg, SUB, LANES))
    ref[0] = jnp.where(lane >= z.ny, rolled(ref[z.xl], z.ny), 0.0)
    ref[z.xl + 1] = jnp.where(lane < LANES - z.ny, rolled(ref[1], -z.ny), 0.0)


def beside(z, ref, x, lane_y):
    c = ref[x + 1]
    west = jnp.where(lane_y > 0, rolled(c, 1), 0.0)
    east = jnp.where(lane_y < z.ny - 1, rolled(c, -1), 0.0)
    return c, (ref[x] + ref[x + 2]) + (west + east)


def swap_blocks(z, src, src_off, dst, dst_off):
    lane = lane_ids((SUB, LANES))

    def one(i, carry):
        xg, r = split2(i, z.rg)
        v = [src[xg * CB + j + src_off, r] for j in range(CB)]
        for bit in (1, 2, 4):
            shift = bit * CB
            low = (lane & shift) == 0
            for j in range(CB):
                if j & bit == 0:
                    a, b = v[j], v[j | bit]
                    v[j] = jnp.where(low, a, rolled(b, shift))
                    v[j | bit] = jnp.where(low, rolled(a, -shift), b)
        for j in range(CB):
            dst[xg * CB + j + dst_off, r] = v[j]
        return carry

    lax.fori_loop(0, z.xl // CB * z.rg, one, 0, unroll=2)


def forward_kernel(z, *refs):
    blocks_ref = refs[0]
    tile_refs = refs[1 : 1 + z.tiles]
    w_ref, pert_ref, cells_ref, column_ref, dep_ref, ow_ref = refs[1 + z.tiles : 7 + z.tiles]
    outs = refs[7 + z.tiles :]
    seen_ref, rate_ref = outs[:2]
    inc_refs = outs[2 : 2 + z.n_mem]
    every, field, other, fine_ref, inc = outs[2 + z.n_mem :]
    me = lax.axis_index("mem")
    for s in range(z.chips):
        every[z.tile_at(s, True, False)] = tile_refs[s][...]
        every[z.tile_at(s, True, True)] = tile_refs[z.chips + s][...]

    group = lane_ids((z.rg, SUB, LANES)) // z.cy
    group_row = lane_ids((SUB, LANES)) // z.cy
    for xl, pieces in enumerate(z.pieces()):
        total, rate = None, None
        for tile, xq, q, to in pieces:
            shift = (to - q) * z.cy
            v = rolled(every[tile, xq * z.rg : (xq + 1) * z.rg], shift)
            w = rolled(jnp.broadcast_to(every[tile, z.t_rows, xq : xq + 1], (SUB, LANES)), shift)
            total = v if total is None else jnp.where(group == to, v, total)
            rate = w if rate is None else jnp.where(group_row == to, w, rate)
        field[xl + 1] = total
        rate_ref[xl] = rate

    lane_y = lane_ids((z.rg, SUB, LANES)) % z.ny
    src, dst = field, other
    for sweep in range(SWEEPS):
        fill_edges(z, src)

        def row(x, carry, src=src, dst=dst):
            c, near = beside(z, src, x, lane_y)
            dst[x + 1] = c + rate_ref[x] * (near - 4.0 * c)
            return carry

        lax.fori_loop(0, z.xl, row, 0, unroll=2)
        src, dst = dst, src
    swap_blocks(z, src, 1, dst, 0)

    lane = lane_ids((z.rows, LANES))
    half = lane // z.block
    pitch = z.rows + PITCH_PAD

    def fine_block(f, carry):
        at, g = z.block_place(blocks_ref[f])
        v = dst[at].reshape(z.rows, LANES)
        v = jnp.where(half == g, v, rolled(v, z.block))
        hi = v.astype(jnp.bfloat16)
        hi32 = hi.astype(jnp.float32)
        first = jnp.where(half == 0, hi32, v - hi32).astype(jnp.bfloat16)
        lhs = jnp.concatenate([first, hi[:, : z.block]], axis=1)
        out = jnp.dot(lhs, w_ref[f], preferred_element_type=jnp.float32)
        start = pl.multiple_of(f * pitch, SUB)
        for t in range(z.ct):
            fine_ref[t, pl.ds(start, z.rows), :] = out[:, t * LANES : (t + 1) * LANES]
        return carry

    lax.fori_loop(0, z.fine, fine_block, 0, unroll=4)

    def level(l, carry):
        for t in range(z.ct):
            cols = slice(t * LANES, (t + 1) * LANES)
            fine = [
                fine_ref[t, pl.ds(m * z.levels + l, z.fine, stride=pitch), :]
                for m in range(z.members)
            ]
            for v in range(z.vars):
                total = None
                for m in range(z.members):
                    term = fine[m] * pert_ref[m, l, v, :, cols].astype(jnp.float32)
                    total = term if total is None else total + term
                inc[l * z.vars + v, :, cols] = total
        return carry

    lax.fori_loop(0, z.levels, level, 0)

    where, _ = split2(cells_ref[...], z.bcells)
    ids = lax.broadcasted_iota(jnp.int32, (z.fine, z.obs), 0)
    here = ids == where
    for l in range(z.levels):
        part = inc[l * z.vars : (l + 1) * z.vars].reshape(z.vars * z.fine, z.bcells)
        hi, lo = hi_lo(part)
        seen = jnp.dot(hi, column_ref[...], preferred_element_type=jnp.float32) + jnp.dot(
            lo, column_ref[...], preferred_element_type=jnp.float32
        )
        for v in range(z.vars):
            s = l * z.vars + v
            got = jnp.where(here, seen[v * z.fine : (v + 1) * z.fine], 0.0)
            seen_ref[s : s + 1, : z.obs] = jnp.sum(got, axis=0, keepdims=True)
    seen_ref[:, z.obs :] = jnp.zeros((z.slabs, LANES), jnp.float32)
    for g in range(z.n_mem):
        mine = slice(g * z.slab_dev, (g + 1) * z.slab_dev)
        seen_ref[mine, : z.obs] -= jnp.where(g == me, dep_ref[...], 0.0)
    for j in range(z.slab_dev):
        for t in range(z.ot):
            at = j * z.ot + t
            seen_ref[at : at + 1, z.obs :] = ow_ref[j : j + 1, t * LANES : (t + 1) * LANES]
    for s in range(z.n_mem):
        to = lax.rem(me + s, z.n_mem)
        for j in range(z.slab_dev):
            inc_refs[s][j] = inc[to * z.slab_dev + j]


def adjoint_kernel(z, *refs):
    blocks_ref, count_ref = refs[:2]
    seen_refs = refs[2 : 2 + z.n_mem]
    w_ref, pert_ref, cells_ref, column_ref, rate_ref = refs[2 + z.n_mem : 7 + z.n_mem]
    out_ref, keep_ref, send_ref = refs[7 + z.n_mem : 10 + z.n_mem]
    every, field, other, fine_ref, force, obs_w = refs[10 + z.n_mem :]
    me = lax.axis_index("mem")
    total = None
    for s in range(z.n_mem):
        part = seen_refs[s][:, : z.obs]
        total = part if total is None else total + part
        obs_w[lax.rem(me + (z.n_mem - s), z.n_mem)] = seen_refs[s][:, z.obs :]
    used = lane_ids((1, z.obs)) < count_ref[0, 0]
    where, _ = split2(cells_ref[...], z.bcells)
    ids = lax.broadcasted_iota(jnp.int32, (z.fine, z.obs), 0)
    here = ids == where
    rows = []
    for s in range(z.slabs):
        g, j = divmod(s, z.slab_dev)
        w = jnp.concatenate([obs_w[g, j * z.ot + t : j * z.ot + t + 1] for t in range(z.ot)], axis=1)
        rows.append(jnp.where(used, w * total[s : s + 1], 0.0))
    for j in range(z.slab_dev):
        mine = rows[j]
        for g in range(1, z.n_mem):
            mine = jnp.where(g == me, rows[g * z.slab_dev + j], mine)
        out_ref[j : j + 1] = mine
    dims = (((1,), (1,)), ((), ()))
    for l in range(z.levels):
        his, los = [], []
        for v in range(z.vars):
            row = jnp.where(here, rows[l * z.vars + v], 0.0)
            hi, lo = hi_lo(row)
            his.append(hi)
            los.append(lo)
        part = lax.dot_general(
            jnp.concatenate(his, axis=0), column_ref[...], dims, preferred_element_type=jnp.float32
        ) + lax.dot_general(
            jnp.concatenate(los, axis=0), column_ref[...], dims, preferred_element_type=jnp.float32
        )
        force[l * z.vars : (l + 1) * z.vars] = part.reshape(z.vars, z.fine, z.bcells)

    pitch = z.fine + PITCH_PAD

    def level(l, carry):
        for t in range(z.ct):
            cols = slice(t * LANES, (t + 1) * LANES)
            f = [force[l * z.vars + v, :, cols] for v in range(z.vars)]
            for m in range(z.members):
                grad = None
                for v in range(z.vars):
                    term = f[v] * pert_ref[m, l, v, :, cols].astype(jnp.float32)
                    grad = term if grad is None else grad + term
                start = pl.multiple_of((m * z.levels + l) * pitch, SUB)
                fine_ref[t, pl.ds(start, z.fine), :] = grad
        return carry

    lax.fori_loop(0, z.levels, level, 0)
    other[...] = jnp.zeros(other.shape, jnp.float32)
    half = lane_ids((z.rows, LANES)) // z.block

    def fine_block(f, carry):
        at, g = z.block_place(blocks_ref[f])
        grad = jnp.concatenate(
            [fine_ref[t, pl.ds(f, z.rows, stride=pitch), :] for t in range(z.ct)], axis=1
        )
        hi, lo = hi_lo(grad)
        out = lax.dot_general(
            jnp.concatenate([hi, lo], axis=0),
            w_ref[f, z.block :, :],
            dims,
            preferred_element_type=jnp.float32,
        )
        out = out[: z.rows] + out[z.rows :]
        out = out + rolled(out, z.block)
        out = jnp.where(half == g, out, 0.0)
        other[at] += out.reshape(z.rg, SUB, LANES)
        return carry

    lax.fori_loop(0, z.fine, fine_block, 0, unroll=4)
    swap_blocks(z, other, 0, field, 1)

    lane_y = lane_ids((z.rg, SUB, LANES)) % z.ny
    for sweep in range(SWEEPS):

        def scale(x, carry):
            other[x + 1] = rate_ref[x] * field[x + 1]
            return carry

        lax.fori_loop(0, z.xl, scale, 0, unroll=4)
        fill_edges(z, other)

        def row(x, carry):
            c, near = beside(z, other, x, lane_y)
            field[x + 1] = field[x + 1] + near - 4.0 * c
            return carry

        lax.fori_loop(0, z.xl, row, 0, unroll=2)

    group = lane_ids((z.rg, SUB, LANES)) // z.cy
    packed = {}
    for xl, pieces in enumerate(z.pieces()):
        for tile, xq, q, to in pieces:
            packed.setdefault((tile, xq), []).append((xl, q, to))
    for (tile, xq), parts in packed.items():
        total = None
        for xl, q, to in parts:
            v = rolled(field[xl + 1], (q - to) * z.cy)
            total = v if total is None else jnp.where(group == q, v, total)
        every[tile, xq * z.rg : (xq + 1) * z.rg] = total
    for s in range(z.chips):
        keep_ref[s] = every[z.tile_at(s, False, False)]
        send_ref[s] = every[z.tile_at(s, False, True)]


def finish_kernel(z, alpha_ref, *refs):
    out_ref = refs[-1]
    total = refs[0][...]
    for ref in refs[1:-1]:
        total = total + ref[...]
    for x in range(z.cx):
        q, xq = divmod(x, z.xq)
        part = total[xq * z.rg : (xq + 1) * z.rg, :, q * z.cy : (q + 1) * z.cy]
        out_ref[:, x, :] = alpha_ref[:, x, :] + part.reshape(z.rows, z.cy)


def on_device(
    alpha,
    filter_rate,
    block_list,
    interp_weights,
    perturbations,
    obs_cells,
    obs_count,
    departures,
    obs_weight,
):
    z = Sizes(alpha, interp_weights, perturbations, obs_cells, departures)
    f32, bf16 = jnp.float32, jnp.bfloat16
    shape = jax.ShapeDtypeStruct
    coarse = alpha.reshape(z.rows, z.cx, z.cy)
    wanted = block_list.reshape(z.fine)
    weights = interp_weights.reshape(z.fine, z.block, z.bcells)
    cells = obs_cells.reshape(1, z.obs)
    dep = departures.reshape(z.slab_dev, z.obs)
    ow = obs_weight.reshape(z.slab_dev, z.obs)
    axes = ("tx", "ty")
    tile_shape = (z.t_rows, SUB, LANES)
    full_shape = (z.t_rows + 1, SUB, LANES)
    grid_shape = (z.xl + 2, z.rg, SUB, LANES)

    own = pl.pallas_call(
        functools.partial(pack_kernel, z),
        out_shape=shape(full_shape, f32),
        in_specs=[VM, VM],
        out_specs=VM,
        compiler_params=params(8),
        name="pack",
    )(coarse, filter_rate)
    tiles = [own] + [lax.ppermute(own, axes, z.chip_perm(s)) for s in range(1, z.chips)]
    tiles += [lax.ppermute(t, axes, z.core_perm()) for t in tiles]

    stacked, column = pl.pallas_call(
        functools.partial(prep_kernel, z),
        out_shape=(
            shape((z.fine, 3 * z.block, z.bcells), bf16),
            shape((z.bcells, z.obs), bf16),
        ),
        in_specs=[VM, VM],
        out_specs=(VM, VM),
        compiler_params=params(16),
        cost_estimate=pl.CostEstimate(flops=4_000_000, bytes_accessed=5_000_000, transcendentals=0),
        name="prep",
    )(weights, cells)

    pitch = z.rows + PITCH_PAD
    slab_shape = (z.slab_dev, z.fine, z.bcells)
    outs = pl.pallas_call(
        functools.partial(forward_kernel, z),
        out_shape=(
            shape((z.slabs, z.obs + LANES), f32),
            shape((z.xl, SUB, LANES), f32),
            *[shape(slab_shape, f32)] * z.n_mem,
        ),
        in_specs=[SM] + [VM] * (z.tiles + 6),
        out_specs=(VM,) * (2 + z.n_mem),
        scratch_shapes=[
            pltpu.VMEM((z.tiles, *full_shape), f32),
            pltpu.VMEM(grid_shape, f32),
            pltpu.VMEM(grid_shape, f32),
            pltpu.VMEM((z.ct, z.fine * pitch, LANES), f32),
            pltpu.VMEM((z.slabs, z.fine, z.bcells), f32),
        ],
        compiler_params=params(24),
        cost_estimate=pl.CostEstimate(flops=20_000_000, bytes_accessed=8_000_000, transcendentals=0),
        name="forward",
    )(wanted, *tiles, stacked, perturbations, cells, column, dep, ow)
    seen, rate, incs = outs[0], outs[1], outs[2:]

    def ring(step):
        return [(i, (i + step) % z.n_mem) for i in range(z.n_mem)]

    steps = range(1, z.n_mem)
    seens = [seen] + [lax.ppermute(seen, "mem", ring(s)) for s in steps]
    parts = [lax.ppermute(incs[s], "mem", ring(s)) for s in steps]

    pitch = z.fine + PITCH_PAD
    weighted, keep, send = pl.pallas_call(
        functools.partial(adjoint_kernel, z),
        out_shape=(
            shape((z.slab_dev, z.obs), f32),
            shape((z.chips, *tile_shape), f32),
            shape((z.chips, *tile_shape), f32),
        ),
        in_specs=[SM, SM] + [VM] * (z.n_mem + 5),
        out_specs=(VM, VM, VM),
        scratch_shapes=[
            pltpu.VMEM((z.tiles, *tile_shape), f32),
            pltpu.VMEM(grid_shape, f32),
            pltpu.VMEM(grid_shape, f32),
            pltpu.VMEM((z.ct, z.rows * pitch, LANES), f32),
            pltpu.VMEM((z.slabs, z.fine, z.bcells), f32),
            pltpu.VMEM((z.n_mem, z.slabs, LANES), f32),
        ],
        compiler_params=params(24),
        cost_estimate=pl.CostEstimate(flops=20_000_000, bytes_accessed=8_000_000, transcendentals=0),
        name="adjoint",
    )(wanted, obs_count, *seens, stacked, perturbations, cells, column, rate)

    came = lax.ppermute(send, axes, z.core_perm())
    sums = [keep[s] + came[s] for s in range(z.chips)]
    sums = [sums[0]] + [lax.ppermute(sums[s], axes, z.chip_perm(s)) for s in range(1, z.chips)]
    gradient = pl.pallas_call(
        functools.partial(finish_kernel, z),
        out_shape=shape((z.rows, z.cx, z.cy), f32),
        in_specs=[VM] * (1 + z.chips),
        out_specs=VM,
        compiler_params=params(8),
        name="finish",
    )(coarse, *sums)
    increment = incs[0]
    for part in parts:
        increment = increment + part
    return (increment, weighted.reshape(departures.shape), gradient.reshape(alpha.shape))


def solution(mesh):
    return jax.shard_map(
        on_device,
        mesh=mesh,
        in_specs=(
            P("mem", None, "tx", "ty"),
            P("tx", "ty"),
            P("tx", "ty", None),
            P("tx", "ty", None, None, None),
            P("mem", None, None, ("tx", "ty"), None),
            P("tx", "ty", None),
            P("tx", "ty"),
            P("tx", "ty", "mem", None),
            P("tx", "ty", "mem", None),
        ),
        out_specs=(
            P("mem", ("tx", "ty"), None),
            P("tx", "ty", "mem", None),
            P("mem", None, "tx", "ty"),
        ),
        check_vma=False,
    )
```

```python
import functools

import jax
import jax.numpy as jnp
from jax import lax
from jax.experimental import pallas as pl
from jax.experimental.pallas import tpu as pltpu
from jax.sharding import PartitionSpec as P


CB = 8
SWEEPS = 4
LANES = 128
SUB = 8
PITCH_PAD = 8


VM = pl.BlockSpec(memory_space=pltpu.VMEM)
HB = pl.BlockSpec(memory_space=pltpu.HBM)
SM = pl.BlockSpec(memory_space=pltpu.SMEM)


def params(mib):
    return pltpu.CompilerParams(vmem_limit_bytes=mib << 20)


def split2(v, n):
    if n & (n - 1) == 0:
        return v >> (n.bit_length() - 1), v & (n - 1)
    return lax.div(v, n), lax.rem(v, n)


def hi_lo(v):
    hi = v.astype(jnp.bfloat16)
    return hi, (v - hi.astype(jnp.float32)).astype(jnp.bfloat16)


def lane_ids(shape):
    return lax.broadcasted_iota(jnp.int32, shape, len(shape) - 1)


class Sizes:
    def __init__(self, alpha, weights, perts, cells, departures):
        self.n_tx, self.n_ty, self.n_mem = (lax.axis_size(a) for a in ("tx", "ty", "mem"))
        self.tiles = self.n_tx * self.n_ty
        self.chips = self.tiles // 2
        self.members, self.levels, self.cx, self.cy = alpha.shape
        self.rows = self.members * self.levels
        self.rg = self.rows // SUB
        self.fine, self.block, self.bcells = weights.shape[2:]
        self.vars = perts.shape[2]
        self.slabs = self.levels * self.vars
        self.slab_dev = departures.shape[2]
        self.obs = cells.shape[-1]
        self.nx, self.ny = self.n_tx * self.cx, self.n_ty * self.cy
        self.groups = LANES // self.ny
        self.xl = self.nx // self.groups
        self.nq = LANES // self.cy
        self.xq = self.cx // self.nq
        self.t_rows = self.xq * self.rg
        self.ct = self.bcells // LANES
        self.ot = self.obs // LANES
        self.blk_x, self.blk_y = self.cx // CB, self.cy // CB
        assert self.n_tx % 2 == 0 and self.groups * self.ny == LANES and self.ny == CB * CB
        assert self.xl % CB == 0 and self.nq * self.cy == LANES and self.xq * self.nq == self.cx
        assert self.xq <= SUB and self.rows % SUB == 0 and self.groups == 2
        assert self.slab_dev * self.ot <= self.slabs

    def block_place(self, bid):
        tile, kb = split2(bid, self.blk_x * self.blk_y)
        a, b = split2(tile, self.n_ty)
        bx, by = split2(kb, self.blk_y)
        gx, gy = a * self.blk_x + bx, b * self.blk_y + by
        g, xg = split2(gx, self.xl // CB)
        return xg * CB + gy, g

    def tile_at(self, step, back, other_core):
        tx, ty = lax.axis_index("tx"), lax.axis_index("ty")
        half = self.n_tx // 2
        chip_y, core = split2(tx, 2)
        dy, dx = divmod(step, self.n_ty)
        if back:
            dy, dx = half - dy, self.n_ty - dx
        y = lax.rem(chip_y + dy, half)
        x = lax.rem(ty + dx, self.n_ty)
        if other_core:
            core = 1 - core
        return (y * 2 + core) * self.n_ty + x

    def chip_perm(self, step):
        half = self.n_tx // 2
        dy, dx = divmod(step, self.n_ty)
        pairs = []
        for y in range(half):
            for core in range(2):
                for x in range(self.n_ty):
                    to = ((y + dy) % half * 2 + core) * self.n_ty + (x + dx) % self.n_ty
                    pairs.append(((y * 2 + core) * self.n_ty + x, to))
        return pairs

    def core_perm(self):
        return [(i, (i // self.n_ty ^ 1) * self.n_ty + i % self.n_ty) for i in range(self.tiles)]

    def pieces(self):
        table = [[] for _ in range(self.xl)]
        for a in range(self.n_tx):
            for x in range(self.cx):
                g, xl = divmod(a * self.cx + x, self.xl)
                q, xq = divmod(x, self.xq)
                for b in range(self.n_ty):
                    table[xl].append((a * self.n_ty + b, xq, q, g * self.ny // self.cy + b))
        return table


def rolled(v, shift):
    shift %= LANES
    return v if shift == 0 else pltpu.roll(v, shift, v.ndim - 1)


def pack_kernel(z, alpha_hbm, rate_hbm, out_ref, alpha_ref, rate_ref, sems):
    copies = [
        pltpu.make_async_copy(alpha_hbm, alpha_ref, sems.at[0]),
        pltpu.make_async_copy(rate_hbm, rate_ref, sems.at[1]),
    ]
    for copy in copies:
        copy.start()
    for copy in copies:
        copy.wait()
    out_ref[z.t_rows] = jnp.zeros((SUB, LANES), jnp.float32)
    for x in range(z.cx):
        q, xq = divmod(x, z.xq)
        lanes = slice(q * z.cy, (q + 1) * z.cy)
        v = alpha_ref[:, x, :]
        out_ref[xq * z.rg : (xq + 1) * z.rg, :, lanes] = v.reshape(z.rg, SUB, z.cy)
        out_ref[z.t_rows, xq : xq + 1, lanes] = rate_ref[x : x + 1, :]


def prep_kernel(z, weights_ref, cells_ref, stacked_ref, column_ref):
    k = z.block

    def one(f, carry):
        hi, lo = hi_lo(weights_ref[f])
        stacked_ref[f, 0:k, :] = hi
        stacked_ref[f, k : 2 * k, :] = hi
        stacked_ref[f, 2 * k : 3 * k, :] = lo
        return carry

    lax.fori_loop(0, z.fine, one, 0, unroll=2)
    _, col = split2(cells_ref[...], z.bcells)
    ids = lax.broadcasted_iota(jnp.int32, (z.bcells, z.obs), 0)
    column_ref[...] = jnp.where(ids == col, 1.0, 0.0).astype(jnp.bfloat16)


def fill_edges(z, ref):
    lane = lane_ids((z.rg, SUB, LANES))
    ref[0] = jnp.where(lane >= z.ny, rolled(ref[z.xl], z.ny), 0.0)
    ref[z.xl + 1] = jnp.where(lane < LANES - z.ny, rolled(ref[1], -z.ny), 0.0)


def beside(z, ref, x, lane_y):
    c = ref[x + 1]
    west = jnp.where(lane_y > 0, rolled(c, 1), 0.0)
    east = jnp.where(lane_y < z.ny - 1, rolled(c, -1), 0.0)
    return c, (ref[x] + ref[x + 2]) + (west + east)


def swap_blocks(z, src, src_off, dst, dst_off):
    lane = lane_ids((SUB, LANES))

    def one(i, carry):
        xg, r = split2(i, z.rg)
        v = [src[xg * CB + j + src_off, r] for j in range(CB)]
        for bit in (1, 2, 4):
            shift = bit * CB
            low = (lane & shift) == 0
            for j in range(CB):
                if j & bit == 0:
                    a, b = v[j], v[j | bit]
                    v[j] = jnp.where(low, a, rolled(b, shift))
                    v[j | bit] = jnp.where(low, rolled(a, -shift), b)
        for j in range(CB):
            dst[xg * CB + j + dst_off, r] = v[j]
        return carry

    lax.fori_loop(0, z.xl // CB * z.rg, one, 0, unroll=8)


def forward_kernel(z, *refs):
    blocks_ref = refs[0]
    tile_refs = refs[1 : 1 + z.tiles]
    w_ref, pert_ref, cells_ref, column_ref, dep_ref, ow_ref = refs[1 + z.tiles : 7 + z.tiles]
    outs = refs[7 + z.tiles :]
    seen_ref, rate_ref = outs[:2]
    inc_refs = outs[2 : 2 + z.n_mem]
    every, field, other, fine_ref, inc = outs[2 + z.n_mem :]
    me = lax.axis_index("mem")
    for s in range(z.chips):
        every[z.tile_at(s, True, False)] = tile_refs[s][...]
        every[z.tile_at(s, True, True)] = tile_refs[z.chips + s][...]

    group = lane_ids((z.rg, SUB, LANES)) // z.cy
    group_row = lane_ids((SUB, LANES)) // z.cy
    for xl, pieces in enumerate(z.pieces()):
        total, rate = None, None
        for tile, xq, q, to in pieces:
            shift = (to - q) * z.cy
            v = rolled(every[tile, xq * z.rg : (xq + 1) * z.rg], shift)
            w = rolled(jnp.broadcast_to(every[tile, z.t_rows, xq : xq + 1], (SUB, LANES)), shift)
            total = v if total is None else jnp.where(group == to, v, total)
            rate = w if rate is None else jnp.where(group_row == to, w, rate)
        field[xl + 1] = total
        rate_ref[xl] = rate

    lane_y = lane_ids((z.rg, SUB, LANES)) % z.ny
    src, dst = field, other
    for _ in range(SWEEPS):
        fill_edges(z, src)

        def row(x, carry, src=src, dst=dst):
            c, near = beside(z, src, x, lane_y)
            dst[x + 1] = c + rate_ref[x] * (near - 4.0 * c)
            return carry

        lax.fori_loop(0, z.xl, row, 0, unroll=True)
        src, dst = dst, src
    swap_blocks(z, src, 1, dst, 0)

    lane = lane_ids((z.rows, LANES))
    half = lane // z.block
    pitch = z.rows + PITCH_PAD

    def fine_block(f, carry):
        at, g = z.block_place(blocks_ref[f])
        v = dst[at].reshape(z.rows, LANES)
        v = jnp.where(half == g, v, rolled(v, z.block))
        hi = v.astype(jnp.bfloat16)
        hi32 = hi.astype(jnp.float32)
        first = jnp.where(half == 0, hi32, v - hi32).astype(jnp.bfloat16)
        lhs = jnp.concatenate([first, hi[:, : z.block]], axis=1)
        out = jnp.dot(lhs, w_ref[f], preferred_element_type=jnp.float32)
        start = pl.multiple_of(f * pitch, SUB)
        for t in range(z.ct):
            fine_ref[t, pl.ds(start, z.rows), :] = out[:, t * LANES : (t + 1) * LANES]
        return carry

    lax.fori_loop(0, z.fine, fine_block, 0, unroll=16)

    def level(l, carry):
        for t in range(z.ct):
            cols = slice(t * LANES, (t + 1) * LANES)
            fine = [
                fine_ref[t, pl.ds(m * z.levels + l, z.fine, stride=pitch), :]
                for m in range(z.members)
            ]
            for v in range(z.vars):
                total = None
                for m in range(z.members):
                    term = fine[m] * pert_ref[m, l, v, :, cols].astype(jnp.float32)
                    total = term if total is None else total + term
                inc[l * z.vars + v, :, cols] = total
        return carry

    lax.fori_loop(0, z.levels, level, 0)

    where, _ = split2(cells_ref[...], z.bcells)
    ids = lax.broadcasted_iota(jnp.int32, (z.fine, z.obs), 0)
    here = ids == where
    for l in range(z.levels):
        part = inc[l * z.vars : (l + 1) * z.vars].reshape(z.vars * z.fine, z.bcells)
        hi, lo = hi_lo(part)
        seen = jnp.dot(hi, column_ref[...], preferred_element_type=jnp.float32) + jnp.dot(
            lo, column_ref[...], preferred_element_type=jnp.float32
        )
        for v in range(z.vars):
            s = l * z.vars + v
            got = jnp.where(here, seen[v * z.fine : (v + 1) * z.fine], 0.0)
            seen_ref[s : s + 1, : z.obs] = jnp.sum(got, axis=0, keepdims=True)
    seen_ref[:, z.obs :] = jnp.zeros((z.slabs, LANES), jnp.float32)
    for g in range(z.n_mem):
        mine = slice(g * z.slab_dev, (g + 1) * z.slab_dev)
        seen_ref[mine, : z.obs] -= jnp.where(g == me, dep_ref[...], 0.0)
    for j in range(z.slab_dev):
        for t in range(z.ot):
            at = j * z.ot + t
            seen_ref[at : at + 1, z.obs :] = ow_ref[j : j + 1, t * LANES : (t + 1) * LANES]
    for s in range(z.n_mem):
        to = lax.rem(me + s, z.n_mem)
        for j in range(z.slab_dev):
            inc_refs[s][j] = inc[to * z.slab_dev + j]


def adjoint_kernel(z, *refs):
    blocks_ref, count_ref = refs[:2]
    seen_refs = refs[2 : 2 + z.n_mem]
    w_ref, pert_ref, cells_ref, column_ref, rate_ref = refs[2 + z.n_mem : 7 + z.n_mem]
    out_ref, keep_ref, send_ref = refs[7 + z.n_mem : 10 + z.n_mem]
    every, field, other, fine_ref, force, obs_w = refs[10 + z.n_mem :]
    me = lax.axis_index("mem")
    total = None
    for s in range(z.n_mem):
        part = seen_refs[s][:, : z.obs]
        total = part if total is None else total + part
        obs_w[lax.rem(me + (z.n_mem - s), z.n_mem)] = seen_refs[s][:, z.obs :]
    used = lane_ids((1, z.obs)) < count_ref[0, 0]
    where, _ = split2(cells_ref[...], z.bcells)
    ids = lax.broadcasted_iota(jnp.int32, (z.fine, z.obs), 0)
    here = ids == where
    rows = []
    for s in range(z.slabs):
        g, j = divmod(s, z.slab_dev)
        w = jnp.concatenate([obs_w[g, j * z.ot + t : j * z.ot + t + 1] for t in range(z.ot)], axis=1)
        rows.append(jnp.where(used, w * total[s : s + 1], 0.0))
    for j in range(z.slab_dev):
        mine = rows[j]
        for g in range(1, z.n_mem):
            mine = jnp.where(g == me, rows[g * z.slab_dev + j], mine)
        out_ref[j : j + 1] = mine
    dims = (((1,), (1,)), ((), ()))
    for l in range(z.levels):
        his, los = [], []
        for v in range(z.vars):
            row = jnp.where(here, rows[l * z.vars + v], 0.0)
            hi, lo = hi_lo(row)
            his.append(hi)
            los.append(lo)
        part = lax.dot_general(
            jnp.concatenate(his, axis=0), column_ref[...], dims, preferred_element_type=jnp.float32
        ) + lax.dot_general(
            jnp.concatenate(los, axis=0), column_ref[...], dims, preferred_element_type=jnp.float32
        )
        force[l * z.vars : (l + 1) * z.vars] = part.reshape(z.vars, z.fine, z.bcells)

    pitch = z.fine + PITCH_PAD

    def level(l, carry):
        for t in range(z.ct):
            cols = slice(t * LANES, (t + 1) * LANES)
            f = [force[l * z.vars + v, :, cols] for v in range(z.vars)]
            for m in range(z.members):
                grad = None
                for v in range(z.vars):
                    term = f[v] * pert_ref[m, l, v, :, cols].astype(jnp.float32)
                    grad = term if grad is None else grad + term
                start = pl.multiple_of((m * z.levels + l) * pitch, SUB)
                fine_ref[t, pl.ds(start, z.fine), :] = grad
        return carry

    lax.fori_loop(0, z.levels, level, 0)
    other[...] = jnp.zeros(other.shape, jnp.float32)
    half = lane_ids((z.rows, LANES)) // z.block

    def fine_block(f, carry):
        at, g = z.block_place(blocks_ref[f])
        grad = jnp.concatenate(
            [fine_ref[t, pl.ds(f, z.rows, stride=pitch), :] for t in range(z.ct)], axis=1
        )
        hi, lo = hi_lo(grad)
        out = lax.dot_general(
            jnp.concatenate([hi, lo], axis=0),
            w_ref[f, z.block :, :],
            dims,
            preferred_element_type=jnp.float32,
        )
        out = out[: z.rows] + out[z.rows :]
        out = out + rolled(out, z.block)
        out = jnp.where(half == g, out, 0.0)
        other[at] += out.reshape(z.rg, SUB, LANES)
        return carry

    lax.fori_loop(0, z.fine, fine_block, 0, unroll=16)
    swap_blocks(z, other, 0, field, 1)

    lane_y = lane_ids((z.rg, SUB, LANES)) % z.ny
    for _ in range(SWEEPS):

        def scale(x, carry):
            other[x + 1] = rate_ref[x] * field[x + 1]
            return carry

        lax.fori_loop(0, z.xl, scale, 0, unroll=4)
        fill_edges(z, other)

        def row(x, carry):
            c, near = beside(z, other, x, lane_y)
            field[x + 1] = field[x + 1] + near - 4.0 * c
            return carry

        lax.fori_loop(0, z.xl, row, 0, unroll=True)

    group = lane_ids((z.rg, SUB, LANES)) // z.cy
    packed = {}
    for xl, pieces in enumerate(z.pieces()):
        for tile, xq, q, to in pieces:
            packed.setdefault((tile, xq), []).append((xl, q, to))
    for (tile, xq), parts in packed.items():
        total = None
        for xl, q, to in parts:
            v = rolled(field[xl + 1], (q - to) * z.cy)
            total = v if total is None else jnp.where(group == q, v, total)
        every[tile, xq * z.rg : (xq + 1) * z.rg] = total
    for s in range(z.chips):
        keep_ref[s] = every[z.tile_at(s, False, False)]
        send_ref[s] = every[z.tile_at(s, False, True)]


def finish_kernel(z, alpha_ref, *refs):
    out_ref = refs[-1]
    total = refs[0][...]
    for ref in refs[1:-1]:
        total = total + ref[...]
    for x in range(z.cx):
        q, xq = divmod(x, z.xq)
        part = total[xq * z.rg : (xq + 1) * z.rg, :, q * z.cy : (q + 1) * z.cy]
        out_ref[:, x, :] = alpha_ref[:, x, :] + part.reshape(z.rows, z.cy)


def on_device(
    alpha,
    filter_rate,
    block_list,
    interp_weights,
    perturbations,
    obs_cells,
    obs_count,
    departures,
    obs_weight,
):
    z = Sizes(alpha, interp_weights, perturbations, obs_cells, departures)
    f32, bf16 = jnp.float32, jnp.bfloat16
    shape = jax.ShapeDtypeStruct
    coarse = alpha.reshape(z.rows, z.cx, z.cy)
    wanted = block_list.reshape(z.fine)
    weights = interp_weights.reshape(z.fine, z.block, z.bcells)
    cells = obs_cells.reshape(1, z.obs)
    dep = departures.reshape(z.slab_dev, z.obs)
    ow = obs_weight.reshape(z.slab_dev, z.obs)
    axes = ("tx", "ty")
    tile_shape = (z.t_rows, SUB, LANES)
    full_shape = (z.t_rows + 1, SUB, LANES)
    grid_shape = (z.xl + 2, z.rg, SUB, LANES)

    own = pl.pallas_call(
        functools.partial(pack_kernel, z),
        out_shape=shape(full_shape, f32),
        in_specs=[HB, HB],
        out_specs=VM,
        scratch_shapes=[
            pltpu.VMEM(coarse.shape, f32),
            pltpu.VMEM(filter_rate.shape, f32),
            pltpu.SemaphoreType.DMA((2,)),
        ],
        compiler_params=params(8),
        name="pack",
    )(coarse, filter_rate)
    tiles = [own]
    for s in range(1, z.chips):
        tiles.append(lax.ppermute(own, axes, z.chip_perm(s)))
    for s in range(z.chips):
        tiles.append(lax.ppermute(tiles[s], axes, z.core_perm()))

    stacked, column = pl.pallas_call(
        functools.partial(prep_kernel, z),
        out_shape=(shape((z.fine, 3 * z.block, z.bcells), bf16), shape((z.bcells, z.obs), bf16)),
        in_specs=[VM, VM],
        out_specs=(VM, VM),
        compiler_params=params(16),
        cost_estimate=pl.CostEstimate(flops=4_000_000, bytes_accessed=5_000_000, transcendentals=0),
        name="prep",
    )(weights, cells)

    pitch = z.rows + PITCH_PAD
    slab_shape = (z.slab_dev, z.fine, z.bcells)
    outs = pl.pallas_call(
        functools.partial(forward_kernel, z),
        out_shape=(
            shape((z.slabs, z.obs + LANES), f32),
            shape((z.xl, SUB, LANES), f32),
            *[shape(slab_shape, f32)] * z.n_mem,
        ),
        in_specs=[SM] + [VM] * (z.tiles + 6),
        out_specs=(VM,) * (2 + z.n_mem),
        scratch_shapes=[
            pltpu.VMEM((z.tiles, *full_shape), f32),
            pltpu.VMEM(grid_shape, f32),
            pltpu.VMEM(grid_shape, f32),
            pltpu.VMEM((z.ct, z.fine * pitch, LANES), f32),
            pltpu.VMEM((z.slabs, z.fine, z.bcells), f32),
        ],
        compiler_params=params(24),
        cost_estimate=pl.CostEstimate(flops=20_000_000, bytes_accessed=8_000_000, transcendentals=0),
        name="forward",
    )(wanted, *tiles, stacked, perturbations, cells, column, dep, ow)
    seen, rate, incs = outs[0], outs[1], outs[2:]

    def ring(step):
        return [(i, (i + step) % z.n_mem) for i in range(z.n_mem)]

    steps = range(1, z.n_mem)
    seens, parts = [seen], []
    for s in steps:
        seens.append(lax.ppermute(seen, "mem", ring(s)))
    for s in steps:
        parts.append(lax.ppermute(incs[s], "mem", ring(s)))

    pitch = z.fine + PITCH_PAD
    weighted, keep, send = pl.pallas_call(
        functools.partial(adjoint_kernel, z),
        out_shape=(
            shape((z.slab_dev, z.obs), f32),
            shape((z.chips, *tile_shape), f32),
            shape((z.chips, *tile_shape), f32),
        ),
        in_specs=[SM, SM] + [VM] * (z.n_mem + 5),
        out_specs=(VM, VM, VM),
        scratch_shapes=[
            pltpu.VMEM((z.tiles, *tile_shape), f32),
            pltpu.VMEM(grid_shape, f32),
            pltpu.VMEM(grid_shape, f32),
            pltpu.VMEM((z.ct, z.rows * pitch, LANES), f32),
            pltpu.VMEM((z.slabs, z.fine, z.bcells), f32),
            pltpu.VMEM((z.n_mem, z.slabs, LANES), f32),
        ],
        compiler_params=params(24),
        cost_estimate=pl.CostEstimate(flops=20_000_000, bytes_accessed=8_000_000, transcendentals=0),
        name="adjoint",
    )(wanted, obs_count, *seens, stacked, perturbations, cells, column, rate)

    came = lax.ppermute(send, axes, z.core_perm())
    sums = [keep[s] + came[s] for s in range(z.chips)]
    sums = [sums[0]] + [lax.ppermute(sums[s], axes, z.chip_perm(s)) for s in range(1, z.chips)]
    gradient = pl.pallas_call(
        functools.partial(finish_kernel, z),
        out_shape=shape((z.rows, z.cx, z.cy), f32),
        in_specs=[VM] * (1 + z.chips),
        out_specs=VM,
        compiler_params=params(8),
        name="finish",
    )(coarse, *sums)
    increment = incs[0]
    for part in parts:
        increment = increment + part
    return (increment, weighted.reshape(departures.shape), gradient.reshape(alpha.shape))


def solution(mesh):
    return jax.shard_map(
        on_device,
        mesh=mesh,
        in_specs=(
            P("mem", None, "tx", "ty"),
            P("tx", "ty"),
            P("tx", "ty", None),
            P("tx", "ty", None, None, None),
            P("mem", None, None, ("tx", "ty"), None),
            P("tx", "ty", None),
            P("tx", "ty"),
            P("tx", "ty", "mem", None),
            P("tx", "ty", "mem", None),
        ),
        out_specs=(
            P("mem", ("tx", "ty"), None),
            P("tx", "ty", "mem", None),
            P("mem", None, "tx", "ty"),
        ),
        check_vma=False,
    )
```

```python
import functools

import jax
import jax.numpy as jnp
from jax import lax
from jax.experimental import pallas as pl
from jax.experimental.pallas import tpu as pltpu
from jax.sharding import PartitionSpec as P


CB = 8
SWEEPS = 4
LANES = 128
SUB = 8
PITCH_PAD = 8
PREP_CHUNKS = 4


VM = pl.BlockSpec(memory_space=pltpu.VMEM)
HB = pl.BlockSpec(memory_space=pltpu.HBM)
SM = pl.BlockSpec(memory_space=pltpu.SMEM)


def in_hbm(v):
    return pltpu.with_memory_space_constraint(v, pltpu.HBM)


def params(mib):
    return pltpu.CompilerParams(vmem_limit_bytes=mib << 20)


def split2(v, n):
    if n & (n - 1) == 0:
        return v >> (n.bit_length() - 1), v & (n - 1)
    return lax.div(v, n), lax.rem(v, n)


def hi_lo(v):
    hi = v.astype(jnp.bfloat16)
    return hi, (v - hi.astype(jnp.float32)).astype(jnp.bfloat16)


def lane_ids(shape):
    return lax.broadcasted_iota(jnp.int32, shape, len(shape) - 1)


class Sizes:
    def __init__(self, alpha, weights, perts, cells, departures):
        self.n_tx, self.n_ty, self.n_mem = (lax.axis_size(a) for a in ("tx", "ty", "mem"))
        self.tiles = self.n_tx * self.n_ty
        self.chips = self.tiles // 2
        self.members, self.levels, self.cx, self.cy = alpha.shape
        self.rows = self.members * self.levels
        self.rg = self.rows // SUB
        self.fine, self.block, self.bcells = weights.shape[2:]
        self.vars = perts.shape[2]
        self.slabs = self.levels * self.vars
        self.slab_dev = departures.shape[2]
        self.obs = cells.shape[-1]
        self.nx, self.ny = self.n_tx * self.cx, self.n_ty * self.cy
        self.groups = LANES // self.ny
        self.xl = self.nx // self.groups
        self.nq = LANES // self.cy
        self.xq = self.cx // self.nq
        self.t_rows = self.xq * self.rg
        self.ct = self.bcells // LANES
        self.ot = self.obs // LANES
        self.blk_x, self.blk_y = self.cx // CB, self.cy // CB
        assert self.n_tx % 2 == 0 and self.groups * self.ny == LANES and self.ny == CB * CB
        assert self.xl % CB == 0 and self.nq * self.cy == LANES and self.xq * self.nq == self.cx
        assert self.xq <= SUB and self.rows % SUB == 0 and self.groups == 2
        assert self.slab_dev * self.ot <= self.slabs

    def block_place(self, bid):
        tile, kb = split2(bid, self.blk_x * self.blk_y)
        a, b = split2(tile, self.n_ty)
        bx, by = split2(kb, self.blk_y)
        gx, gy = a * self.blk_x + bx, b * self.blk_y + by
        g, xg = split2(gx, self.xl // CB)
        return xg * CB + gy, g

    def tile_at(self, step, back, other_core):
        tx, ty = lax.axis_index("tx"), lax.axis_index("ty")
        half = self.n_tx // 2
        chip_y, core = split2(tx, 2)
        dy, dx = divmod(step, self.n_ty)
        if back:
            dy, dx = half - dy, self.n_ty - dx
        y = lax.rem(chip_y + dy, half)
        x = lax.rem(ty + dx, self.n_ty)
        if other_core:
            core = 1 - core
        return (y * 2 + core) * self.n_ty + x

    def chip_perm(self, step):
        half = self.n_tx // 2
        dy, dx = divmod(step, self.n_ty)
        pairs = []
        for y in range(half):
            for core in range(2):
                for x in range(self.n_ty):
                    to = ((y + dy) % half * 2 + core) * self.n_ty + (x + dx) % self.n_ty
                    pairs.append(((y * 2 + core) * self.n_ty + x, to))
        return pairs

    def core_perm(self):
        return [(i, (i // self.n_ty ^ 1) * self.n_ty + i % self.n_ty) for i in range(self.tiles)]

    def pieces(self):
        table = [[] for _ in range(self.xl)]
        for a in range(self.n_tx):
            for x in range(self.cx):
                g, xl = divmod(a * self.cx + x, self.xl)
                q, xq = divmod(x, self.xq)
                for b in range(self.n_ty):
                    table[xl].append((a * self.n_ty + b, xq, q, g * self.ny // self.cy + b))
        return table


def rolled(v, shift):
    shift %= LANES
    return v if shift == 0 else pltpu.roll(v, shift, v.ndim - 1)


def pack_kernel(z, alpha_hbm, rate_hbm, out_ref, alpha_ref, rate_ref, sems):
    copies = [
        pltpu.make_async_copy(alpha_hbm, alpha_ref, sems.at[0]),
        pltpu.make_async_copy(rate_hbm, rate_ref, sems.at[1]),
    ]
    for copy in copies:
        copy.start()
    for copy in copies:
        copy.wait()
    out_ref[z.t_rows] = jnp.zeros((SUB, LANES), jnp.float32)
    for x in range(z.cx):
        q, xq = divmod(x, z.xq)
        lanes = slice(q * z.cy, (q + 1) * z.cy)
        v = alpha_ref[:, x, :]
        out_ref[xq * z.rg : (xq + 1) * z.rg, :, lanes] = v.reshape(z.rg, SUB, z.cy)
        out_ref[z.t_rows, xq : xq + 1, lanes] = rate_ref[x : x + 1, :]


def prep_kernel(z, *refs):
    weights_hbm, cells_hbm, count_ref, stacked_ref, column_ref, used_ref = refs[:6]
    weights_ref, cells_ref, sems = refs[6:]
    k = z.block
    chunk = z.fine // PREP_CHUNKS
    copies = []
    for i in range(PREP_CHUNKS):
        part = pl.ds(i * chunk, chunk)
        copies.append(
            pltpu.make_async_copy(weights_hbm.at[part], weights_ref.at[part], sems.at[i])
        )
    cells_copy = pltpu.make_async_copy(cells_hbm, cells_ref, sems.at[PREP_CHUNKS])
    for copy in [cells_copy] + copies:
        copy.start()
    used_ref[...] = jnp.where(lane_ids((1, z.obs)) < count_ref[0, 0], 1.0, 0.0)
    cells_copy.wait()
    _, col = split2(cells_ref[...], z.bcells)
    ids = lax.broadcasted_iota(jnp.int32, (z.bcells, z.obs), 0)
    column_ref[...] = jnp.where(ids == col, 1.0, 0.0).astype(jnp.bfloat16)

    def one(f, carry):
        hi, lo = hi_lo(weights_ref[f])
        stacked_ref[f, 0:k, :] = hi
        stacked_ref[f, k : 2 * k, :] = hi
        stacked_ref[f, 2 * k : 3 * k, :] = lo
        return carry

    for i in range(PREP_CHUNKS):
        copies[i].wait()
        lax.fori_loop(i * chunk, (i + 1) * chunk, one, 0, unroll=2)


def fill_edges(z, ref):
    lane = lane_ids((z.rg, SUB, LANES))
    ref[0] = jnp.where(lane >= z.ny, rolled(ref[z.xl], z.ny), 0.0)
    ref[z.xl + 1] = jnp.where(lane < LANES - z.ny, rolled(ref[1], -z.ny), 0.0)


def beside(z, ref, x, lane_y):
    c = ref[x + 1]
    west = jnp.where(lane_y > 0, rolled(c, 1), 0.0)
    east = jnp.where(lane_y < z.ny - 1, rolled(c, -1), 0.0)
    return c, (ref[x] + ref[x + 2]) + (west + east)


def swap_blocks(z, src, src_off, dst, dst_off):
    lane = lane_ids((SUB, LANES))

    def one(i, carry):
        xg, r = split2(i, z.rg)
        v = [src[xg * CB + j + src_off, r] for j in range(CB)]
        for bit in (1, 2, 4):
            shift = bit * CB
            low = (lane & shift) == 0
            for j in range(CB):
                if j & bit == 0:
                    a, b = v[j], v[j | bit]
                    v[j] = jnp.where(low, a, rolled(b, shift))
                    v[j | bit] = jnp.where(low, rolled(a, -shift), b)
        for j in range(CB):
            dst[xg * CB + j + dst_off, r] = v[j]
        return carry

    lax.fori_loop(0, z.xl // CB * z.rg, one, 0, unroll=8)


def forward_kernel(z, *refs):
    blocks_ref = refs[0]
    tile_refs = refs[1 : 1 + z.tiles]
    w_ref, pert_ref, cells_ref, column_ref, dep_ref, ow_ref = refs[1 + z.tiles : 7 + z.tiles]
    outs = refs[7 + z.tiles :]
    seen_ref, rate_ref = outs[:2]
    inc_refs = outs[2 : 2 + z.n_mem]
    every, field, other, fine_ref, inc = outs[2 + z.n_mem :]
    me = lax.axis_index("mem")
    for s in range(z.chips):
        every[z.tile_at(s, True, False)] = tile_refs[s][...]
        every[z.tile_at(s, True, True)] = tile_refs[z.chips + s][...]

    group = lane_ids((z.rg, SUB, LANES)) // z.cy
    group_row = lane_ids((SUB, LANES)) // z.cy
    for xl, pieces in enumerate(z.pieces()):
        total, rate = None, None
        for tile, xq, q, to in pieces:
            shift = (to - q) * z.cy
            v = rolled(every[tile, xq * z.rg : (xq + 1) * z.rg], shift)
            w = rolled(jnp.broadcast_to(every[tile, z.t_rows, xq : xq + 1], (SUB, LANES)), shift)
            total = v if total is None else jnp.where(group == to, v, total)
            rate = w if rate is None else jnp.where(group_row == to, w, rate)
        field[xl + 1] = total
        rate_ref[xl] = rate

    lane_y = lane_ids((z.rg, SUB, LANES)) % z.ny
    src, dst = field, other
    for _ in range(SWEEPS):
        fill_edges(z, src)

        def row(x, carry, src=src, dst=dst):
            c, near = beside(z, src, x, lane_y)
            dst[x + 1] = c + rate_ref[x] * (near - 4.0 * c)
            return carry

        lax.fori_loop(0, z.xl, row, 0, unroll=True)
        src, dst = dst, src
    swap_blocks(z, src, 1, dst, 0)

    lane = lane_ids((z.rows, LANES))
    half = lane // z.block
    pitch = z.rows + PITCH_PAD

    def fine_block(f, carry):
        at, g = z.block_place(blocks_ref[f])
        v = dst[at].reshape(z.rows, LANES)
        v = jnp.where(half == g, v, rolled(v, z.block))
        hi = v.astype(jnp.bfloat16)
        hi32 = hi.astype(jnp.float32)
        first = jnp.where(half == 0, hi32, v - hi32).astype(jnp.bfloat16)
        lhs = jnp.concatenate([first, hi[:, : z.block]], axis=1)
        out = jnp.dot(lhs, w_ref[f], preferred_element_type=jnp.float32)
        start = pl.multiple_of(f * pitch, SUB)
        for t in range(z.ct):
            fine_ref[t, pl.ds(start, z.rows), :] = out[:, t * LANES : (t + 1) * LANES]
        return carry

    lax.fori_loop(0, z.fine, fine_block, 0, unroll=16)

    def level(l, carry):
        for t in range(z.ct):
            cols = slice(t * LANES, (t + 1) * LANES)
            fine = [
                fine_ref[t, pl.ds(m * z.levels + l, z.fine, stride=pitch), :]
                for m in range(z.members)
            ]
            for v in range(z.vars):
                total = None
                for m in range(z.members):
                    term = fine[m] * pert_ref[m, l, v, :, cols].astype(jnp.float32)
                    total = term if total is None else total + term
                inc[l * z.vars + v, :, cols] = total
        return carry

    lax.fori_loop(0, z.levels, level, 0)

    where, _ = split2(cells_ref[...], z.bcells)
    ids = lax.broadcasted_iota(jnp.int32, (z.fine, z.obs), 0)
    here = ids == where
    for l in range(z.levels):
        part = inc[l * z.vars : (l + 1) * z.vars].reshape(z.vars * z.fine, z.bcells)
        hi, lo = hi_lo(part)
        seen = jnp.dot(hi, column_ref[...], preferred_element_type=jnp.float32) + jnp.dot(
            lo, column_ref[...], preferred_element_type=jnp.float32
        )
        for v in range(z.vars):
            s = l * z.vars + v
            got = jnp.where(here, seen[v * z.fine : (v + 1) * z.fine], 0.0)
            seen_ref[s : s + 1, : z.obs] = jnp.sum(got, axis=0, keepdims=True)
    seen_ref[:, z.obs :] = jnp.zeros((z.slabs, LANES), jnp.float32)
    for g in range(z.n_mem):
        mine = slice(g * z.slab_dev, (g + 1) * z.slab_dev)
        seen_ref[mine, : z.obs] -= jnp.where(g == me, dep_ref[...], 0.0)
    for j in range(z.slab_dev):
        for t in range(z.ot):
            at = j * z.ot + t
            seen_ref[at : at + 1, z.obs :] = ow_ref[j : j + 1, t * LANES : (t + 1) * LANES]
    for s in range(z.n_mem):
        to = lax.rem(me + s, z.n_mem)
        for j in range(z.slab_dev):
            inc_refs[s][j] = inc[to * z.slab_dev + j]


def adjoint_kernel(z, *refs):
    blocks_ref, used_ref = refs[:2]
    seen_refs = refs[2 : 2 + z.n_mem]
    w_ref, pert_ref, cells_ref, column_ref, rate_ref = refs[2 + z.n_mem : 7 + z.n_mem]
    out_ref, keep_ref, send_ref = refs[7 + z.n_mem : 10 + z.n_mem]
    every, field, other, fine_ref, force, obs_w = refs[10 + z.n_mem :]
    me = lax.axis_index("mem")
    total = None
    for s in range(z.n_mem):
        part = seen_refs[s][:, : z.obs]
        total = part if total is None else total + part
        obs_w[lax.rem(me + (z.n_mem - s), z.n_mem)] = seen_refs[s][:, z.obs :]
    used = used_ref[...] > 0.5
    where, _ = split2(cells_ref[...], z.bcells)
    ids = lax.broadcasted_iota(jnp.int32, (z.fine, z.obs), 0)
    here = ids == where
    rows = []
    for s in range(z.slabs):
        g, j = divmod(s, z.slab_dev)
        w = jnp.concatenate([obs_w[g, j * z.ot + t : j * z.ot + t + 1] for t in range(z.ot)], axis=1)
        rows.append(jnp.where(used, w * total[s : s + 1], 0.0))
    for j in range(z.slab_dev):
        mine = rows[j]
        for g in range(1, z.n_mem):
            mine = jnp.where(g == me, rows[g * z.slab_dev + j], mine)
        out_ref[j : j + 1] = mine
    dims = (((1,), (1,)), ((), ()))
    for l in range(z.levels):
        his, los = [], []
        for v in range(z.vars):
            row = jnp.where(here, rows[l * z.vars + v], 0.0)
            hi, lo = hi_lo(row)
            his.append(hi)
            los.append(lo)
        part = lax.dot_general(
            jnp.concatenate(his, axis=0), column_ref[...], dims, preferred_element_type=jnp.float32
        ) + lax.dot_general(
            jnp.concatenate(los, axis=0), column_ref[...], dims, preferred_element_type=jnp.float32
        )
        force[l * z.vars : (l + 1) * z.vars] = part.reshape(z.vars, z.fine, z.bcells)

    pitch = z.fine + PITCH_PAD

    def level(l, carry):
        for t in range(z.ct):
            cols = slice(t * LANES, (t + 1) * LANES)
            f = [force[l * z.vars + v, :, cols] for v in range(z.vars)]
            for m in range(z.members):
                grad = None
                for v in range(z.vars):
                    term = f[v] * pert_ref[m, l, v, :, cols].astype(jnp.float32)
                    grad = term if grad is None else grad + term
                start = pl.multiple_of((m * z.levels + l) * pitch, SUB)
                fine_ref[t, pl.ds(start, z.fine), :] = grad
        return carry

    lax.fori_loop(0, z.levels, level, 0)
    other[...] = jnp.zeros(other.shape, jnp.float32)
    half = lane_ids((z.rows, LANES)) // z.block

    def fine_block(f, carry):
        at, g = z.block_place(blocks_ref[f])
        grad = jnp.concatenate(
            [fine_ref[t, pl.ds(f, z.rows, stride=pitch), :] for t in range(z.ct)], axis=1
        )
        hi, lo = hi_lo(grad)
        out = lax.dot_general(
            jnp.concatenate([hi, lo], axis=0),
            w_ref[f, z.block :, :],
            dims,
            preferred_element_type=jnp.float32,
        )
        out = out[: z.rows] + out[z.rows :]
        out = out + rolled(out, z.block)
        out = jnp.where(half == g, out, 0.0)
        other[at] += out.reshape(z.rg, SUB, LANES)
        return carry

    lax.fori_loop(0, z.fine, fine_block, 0, unroll=16)
    swap_blocks(z, other, 0, field, 1)

    lane_y = lane_ids((z.rg, SUB, LANES)) % z.ny
    for _ in range(SWEEPS):

        def scale(x, carry):
            other[x + 1] = rate_ref[x] * field[x + 1]
            return carry

        lax.fori_loop(0, z.xl, scale, 0, unroll=4)
        fill_edges(z, other)

        def row(x, carry):
            c, near = beside(z, other, x, lane_y)
            field[x + 1] = field[x + 1] + near - 4.0 * c
            return carry

        lax.fori_loop(0, z.xl, row, 0, unroll=True)

    group = lane_ids((z.rg, SUB, LANES)) // z.cy
    packed = {}
    for xl, pieces in enumerate(z.pieces()):
        for tile, xq, q, to in pieces:
            packed.setdefault((tile, xq), []).append((xl, q, to))
    for (tile, xq), parts in packed.items():
        total = None
        for xl, q, to in parts:
            v = rolled(field[xl + 1], (q - to) * z.cy)
            total = v if total is None else jnp.where(group == q, v, total)
        every[tile, xq * z.rg : (xq + 1) * z.rg] = total
    for s in range(z.chips):
        keep_ref[s] = every[z.tile_at(s, False, False)]
        send_ref[s] = every[z.tile_at(s, False, True)]


def finish_kernel(z, alpha_ref, *refs):
    out_ref = refs[-1]
    total = refs[0][...]
    for ref in refs[1:-1]:
        total = total + ref[...]
    for x in range(z.cx):
        q, xq = divmod(x, z.xq)
        part = total[xq * z.rg : (xq + 1) * z.rg, :, q * z.cy : (q + 1) * z.cy]
        out_ref[:, x, :] = alpha_ref[:, x, :] + part.reshape(z.rows, z.cy)


def on_device(
    alpha,
    filter_rate,
    block_list,
    interp_weights,
    perturbations,
    obs_cells,
    obs_count,
    departures,
    obs_weight,
):
    z = Sizes(alpha, interp_weights, perturbations, obs_cells, departures)
    f32, bf16 = jnp.float32, jnp.bfloat16
    shape = jax.ShapeDtypeStruct
    coarse = alpha.reshape(z.rows, z.cx, z.cy)
    wanted = block_list.reshape(z.fine)
    weights = interp_weights.reshape(z.fine, z.block, z.bcells)
    cells = obs_cells.reshape(1, z.obs)
    dep = departures.reshape(z.slab_dev, z.obs)
    ow = obs_weight.reshape(z.slab_dev, z.obs)
    axes = ("tx", "ty")
    tile_shape = (z.t_rows, SUB, LANES)
    full_shape = (z.t_rows + 1, SUB, LANES)
    grid_shape = (z.xl + 2, z.rg, SUB, LANES)

    own = pl.pallas_call(
        functools.partial(pack_kernel, z),
        out_shape=shape(full_shape, f32),
        in_specs=[HB, HB],
        out_specs=VM,
        scratch_shapes=[
            pltpu.VMEM(coarse.shape, f32),
            pltpu.VMEM(filter_rate.shape, f32),
            pltpu.SemaphoreType.DMA((2,)),
        ],
        compiler_params=params(8),
        name="pack",
    )(in_hbm(coarse), in_hbm(filter_rate))
    tiles = [own]
    for s in range(1, z.chips):
        tiles.append(lax.ppermute(own, axes, z.chip_perm(s)))
    for s in range(z.chips):
        tiles.append(lax.ppermute(tiles[s], axes, z.core_perm()))

    stacked, column, used = pl.pallas_call(
        functools.partial(prep_kernel, z),
        out_shape=(
            shape((z.fine, 3 * z.block, z.bcells), bf16),
            shape((z.bcells, z.obs), bf16),
            shape((1, z.obs), f32),
        ),
        in_specs=[HB, HB, SM],
        out_specs=(VM, VM, VM),
        scratch_shapes=[
            pltpu.VMEM(weights.shape, f32),
            pltpu.VMEM(cells.shape, jnp.int32),
            pltpu.SemaphoreType.DMA((PREP_CHUNKS + 1,)),
        ],
        compiler_params=params(16),
        cost_estimate=pl.CostEstimate(flops=4_000_000, bytes_accessed=5_000_000, transcendentals=0),
        name="prep",
    )(in_hbm(weights), in_hbm(cells), obs_count)

    pitch = z.rows + PITCH_PAD
    slab_shape = (z.slab_dev, z.fine, z.bcells)
    outs = pl.pallas_call(
        functools.partial(forward_kernel, z),
        out_shape=(
            shape((z.slabs, z.obs + LANES), f32),
            shape((z.xl, SUB, LANES), f32),
            *[shape(slab_shape, f32)] * z.n_mem,
        ),
        in_specs=[SM] + [VM] * (z.tiles + 6),
        out_specs=(VM,) * (2 + z.n_mem),
        scratch_shapes=[
            pltpu.VMEM((z.tiles, *full_shape), f32),
            pltpu.VMEM(grid_shape, f32),
            pltpu.VMEM(grid_shape, f32),
            pltpu.VMEM((z.ct, z.fine * pitch, LANES), f32),
            pltpu.VMEM((z.slabs, z.fine, z.bcells), f32),
        ],
        compiler_params=params(24),
        cost_estimate=pl.CostEstimate(flops=20_000_000, bytes_accessed=8_000_000, transcendentals=0),
        name="forward",
    )(wanted, *tiles, stacked, perturbations, cells, column, dep, ow)
    seen, rate, incs = outs[0], outs[1], outs[2:]

    def ring(step):
        return [(i, (i + step) % z.n_mem) for i in range(z.n_mem)]

    steps = range(1, z.n_mem)
    seens, parts = [seen], []
    for s in steps:
        seens.append(lax.ppermute(seen, "mem", ring(s)))
    for s in steps:
        parts.append(lax.ppermute(incs[s], "mem", ring(s)))

    pitch = z.fine + PITCH_PAD
    weighted, keep, send = pl.pallas_call(
        functools.partial(adjoint_kernel, z),
        out_shape=(
            shape((z.slab_dev, z.obs), f32),
            shape((z.chips, *tile_shape), f32),
            shape((z.chips, *tile_shape), f32),
        ),
        in_specs=[SM] + [VM] * (z.n_mem + 6),
        out_specs=(VM, VM, VM),
        scratch_shapes=[
            pltpu.VMEM((z.tiles, *tile_shape), f32),
            pltpu.VMEM(grid_shape, f32),
            pltpu.VMEM(grid_shape, f32),
            pltpu.VMEM((z.ct, z.rows * pitch, LANES), f32),
            pltpu.VMEM((z.slabs, z.fine, z.bcells), f32),
            pltpu.VMEM((z.n_mem, z.slabs, LANES), f32),
        ],
        compiler_params=params(24),
        cost_estimate=pl.CostEstimate(flops=20_000_000, bytes_accessed=8_000_000, transcendentals=0),
        name="adjoint",
    )(wanted, used, *seens, stacked, perturbations, cells, column, rate)

    came = lax.ppermute(send, axes, z.core_perm())
    sums = [keep[s] + came[s] for s in range(z.chips)]
    sums = [sums[0]] + [lax.ppermute(sums[s], axes, z.chip_perm(s)) for s in range(1, z.chips)]
    gradient = pl.pallas_call(
        functools.partial(finish_kernel, z),
        out_shape=shape((z.rows, z.cx, z.cy), f32),
        in_specs=[VM] * (1 + z.chips),
        out_specs=VM,
        compiler_params=params(8),
        name="finish",
    )(coarse, *sums)
    increment = incs[0]
    for part in parts:
        increment = increment + part
    return (increment, weighted.reshape(departures.shape), gradient.reshape(alpha.shape))


def solution(mesh):
    return jax.shard_map(
        on_device,
        mesh=mesh,
        in_specs=(
            P("mem", None, "tx", "ty"),
            P("tx", "ty"),
            P("tx", "ty", None),
            P("tx", "ty", None, None, None),
            P("mem", None, None, ("tx", "ty"), None),
            P("tx", "ty", None),
            P("tx", "ty"),
            P("tx", "ty", "mem", None),
            P("tx", "ty", "mem", None),
        ),
        out_specs=(
            P("mem", ("tx", "ty"), None),
            P("tx", "ty", "mem", None),
            P("mem", None, "tx", "ty"),
        ),
        check_vma=False,
    )
```

```python
import functools

import jax
import jax.numpy as jnp
from jax import lax
from jax.experimental import pallas as pl
from jax.experimental.pallas import tpu as pltpu
from jax.sharding import PartitionSpec as P


CB = 8
SWEEPS = 4
LANES = 128
SUB = 8
PITCH_PAD = 8
PREP_CHUNKS = 4
SWAP_UNROLL = 16


VM = pl.BlockSpec(memory_space=pltpu.VMEM)
HB = pl.BlockSpec(memory_space=pltpu.HBM)
SM = pl.BlockSpec(memory_space=pltpu.SMEM)


def in_hbm(v):
    return pltpu.with_memory_space_constraint(v, pltpu.HBM)


def params(mib):
    return pltpu.CompilerParams(vmem_limit_bytes=mib << 20)


def split2(v, n):
    if n & (n - 1) == 0:
        return v >> (n.bit_length() - 1), v & (n - 1)
    return lax.div(v, n), lax.rem(v, n)


def hi_lo(v):
    hi = v.astype(jnp.bfloat16)
    return hi, (v - hi.astype(jnp.float32)).astype(jnp.bfloat16)


def lane_ids(shape):
    return lax.broadcasted_iota(jnp.int32, shape, len(shape) - 1)


class Sizes:
    def __init__(self, alpha, weights, perts, cells, departures):
        self.n_tx, self.n_ty, self.n_mem = (lax.axis_size(a) for a in ("tx", "ty", "mem"))
        self.tiles = self.n_tx * self.n_ty
        self.chips = self.tiles // 2
        self.members, self.levels, self.cx, self.cy = alpha.shape
        self.rows = self.members * self.levels
        self.rg = self.rows // SUB
        self.fine, self.block, self.bcells = weights.shape[2:]
        self.vars = perts.shape[2]
        self.slabs = self.levels * self.vars
        self.slab_dev = departures.shape[2]
        self.obs = cells.shape[-1]
        self.nx, self.ny = self.n_tx * self.cx, self.n_ty * self.cy
        self.halves = LANES // self.ny
        self.hg = self.rg // self.halves
        self.nq = LANES // self.cy
        self.xq = self.cx // self.nq
        self.t_rows = self.xq * self.rg
        self.ct = self.bcells // LANES
        self.ot = self.obs // LANES
        self.blk_x, self.blk_y = self.cx // CB, self.cy // CB
        assert self.n_tx % 2 == 0 and self.halves * self.ny == LANES and self.ny == CB * CB
        assert self.nq * self.cy == LANES and self.xq * self.nq == self.cx and self.xq <= SUB
        assert self.halves == 2 and self.hg * 2 * SUB == self.rows
        assert self.nq == self.halves * self.n_ty
        assert self.slab_dev * self.ot <= self.slabs

    def block_place(self, bid):
        tile, kb = split2(bid, self.blk_x * self.blk_y)
        a, b = split2(tile, self.n_ty)
        bx, by = split2(kb, self.blk_y)
        return (a * self.blk_x + bx) * CB + b * self.blk_y + by

    def tile_at(self, step, back, other_core):
        tx, ty = lax.axis_index("tx"), lax.axis_index("ty")
        half = self.n_tx // 2
        chip_y, core = split2(tx, 2)
        dy, dx = divmod(step, self.n_ty)
        if back:
            dy, dx = half - dy, self.n_ty - dx
        y = lax.rem(chip_y + dy, half)
        x = lax.rem(ty + dx, self.n_ty)
        if other_core:
            core = 1 - core
        return (y * 2 + core) * self.n_ty + x

    def chip_perm(self, step):
        half = self.n_tx // 2
        dy, dx = divmod(step, self.n_ty)
        pairs = []
        for y in range(half):
            for core in range(2):
                for x in range(self.n_ty):
                    to = ((y + dy) % half * 2 + core) * self.n_ty + (x + dx) % self.n_ty
                    pairs.append(((y * 2 + core) * self.n_ty + x, to))
        return pairs

    def core_perm(self):
        return [(i, (i // self.n_ty ^ 1) * self.n_ty + i % self.n_ty) for i in range(self.tiles)]


def rolled(v, shift):
    shift %= LANES
    return v if shift == 0 else pltpu.roll(v, shift, v.ndim - 1)


def pack_kernel(z, alpha_hbm, rate_hbm, out_ref, alpha_ref, rate_ref, sems):
    copies = [
        pltpu.make_async_copy(alpha_hbm, alpha_ref, sems.at[0]),
        pltpu.make_async_copy(rate_hbm, rate_ref, sems.at[1]),
    ]
    for copy in copies:
        copy.start()
    for copy in copies:
        copy.wait()
    rate_rows, tiles = [], []
    for xq in range(z.xq):
        parts = [alpha_ref[:, q * z.xq + xq, :] for q in range(z.nq)]
        tiles.append(jnp.concatenate(parts, axis=1).reshape(z.rg, SUB, LANES))
        parts = [rate_ref[q * z.xq + xq : q * z.xq + xq + 1, :] for q in range(z.nq)]
        rate_rows.append(jnp.concatenate(parts, axis=1))
    b = lax.axis_index("ty")
    for xq in range(z.xq):
        for g in range(z.rg):
            turn = (g // z.hg * z.n_ty + b) * z.cy
            out_ref[xq * z.rg + g] = pltpu.roll(tiles[xq][g], turn, 1)
    rate_rows += [jnp.zeros((SUB - z.xq, LANES), jnp.float32)]
    out_ref[z.t_rows] = pltpu.roll(jnp.concatenate(rate_rows, axis=0), b * z.cy, 1)


def prep_kernel(z, *refs):
    weights_hbm, cells_hbm, count_ref, stacked_ref, column_ref, used_ref = refs[:6]
    weights_ref, cells_ref, sems = refs[6:]
    k = z.block
    chunk = z.fine // PREP_CHUNKS
    copies = []
    for i in range(PREP_CHUNKS):
        part = pl.ds(i * chunk, chunk)
        copies.append(
            pltpu.make_async_copy(weights_hbm.at[part], weights_ref.at[part], sems.at[i])
        )
    cells_copy = pltpu.make_async_copy(cells_hbm, cells_ref, sems.at[PREP_CHUNKS])
    for copy in [cells_copy] + copies:
        copy.start()
    used_ref[...] = jnp.where(lane_ids((1, z.obs)) < count_ref[0, 0], 1.0, 0.0)
    cells_copy.wait()
    _, col = split2(cells_ref[...], z.bcells)
    ids = lax.broadcasted_iota(jnp.int32, (z.bcells, z.obs), 0)
    column_ref[...] = jnp.where(ids == col, 1.0, 0.0).astype(jnp.bfloat16)

    def one(f, carry):
        hi, lo = hi_lo(weights_ref[f])
        stacked_ref[f, 0:k, :] = hi
        stacked_ref[f, k : 2 * k, :] = hi
        stacked_ref[f, 2 * k : 3 * k, :] = lo
        return carry

    for i in range(PREP_CHUNKS):
        copies[i].wait()
        lax.fori_loop(i * chunk, (i + 1) * chunk, one, 0, unroll=2)


def clear_edges(z, ref):
    for x in (0, z.nx + 1):
        ref[x] = jnp.zeros((z.hg, SUB, LANES), jnp.float32)


def sweeps(z, src, dst, rate_ref):
    lane_y = lane_ids((z.hg, SUB, LANES)) % z.ny
    for _ in range(SWEEPS):

        def row(x, carry, src=src, dst=dst):
            c = src[x + 1]
            west = jnp.where(lane_y > 0, rolled(c, 1), 0.0)
            east = jnp.where(lane_y < z.ny - 1, rolled(c, -1), 0.0)
            near = (src[x] + src[x + 2]) + (west + east)
            dst[x + 1] = c + rate_ref[x] * (near - 4.0 * c)
            return carry

        lax.fori_loop(0, z.nx, row, 0, unroll=True)
        src, dst = dst, src
    return src, dst


def swap_blocks(z, src, dst, rate_ref=None):
    lane = lane_ids((SUB, LANES))
    for bit in (1, 2, 4):
        shift = bit * CB
        low = (lane & shift) == 0

        def one(i, carry, src=src, dst=dst):
            bx, r = split2(i, z.hg)
            for j in range(CB):
                if j & bit == 0:
                    at, to = bx * CB + j, bx * CB + (j | bit)
                    a, b = src[at + 1, r], src[to + 1, r]
                    first = jnp.where(low, a, rolled(b, shift))
                    second = jnp.where(low, rolled(a, -shift), b)
                    if rate_ref is not None and bit == 4:
                        first, second = first * rate_ref[at], second * rate_ref[to]
                    dst[at + 1, r] = first
                    dst[to + 1, r] = second
            return carry

        lax.fori_loop(0, z.nx // CB * z.hg, one, 0, unroll=SWAP_UNROLL)
        src, dst = dst, src
    return src, dst


def forward_kernel(z, *refs):
    blocks_ref = refs[0]
    tile_refs = refs[1 : 1 + z.tiles]
    w_ref, pert_ref, cells_ref, column_ref, dep_ref, ow_ref = refs[1 + z.tiles : 7 + z.tiles]
    outs = refs[7 + z.tiles :]
    seen_ref, rate_ref = outs[:2]
    inc_refs = outs[2 : 2 + z.n_mem]
    every, field, other, fine_ref, inc = outs[2 + z.n_mem :]
    me = lax.axis_index("mem")
    for s in range(z.chips):
        every[z.tile_at(s, True, False)] = tile_refs[s][...]
        every[z.tile_at(s, True, True)] = tile_refs[z.chips + s][...]

    clear_edges(z, field)
    clear_edges(z, other)
    group = lane_ids((SUB, LANES)) // z.cy
    for a in range(z.n_tx):
        for q in range(z.nq):
            picks = [divmod((j - q) % z.nq, z.n_ty) for j in range(z.nq)]
            for xq in range(z.xq):
                for r in range(z.hg):
                    total = None
                    for j, (h, b) in enumerate(picks):
                        v = every[a * z.n_ty + b, xq * z.rg + h * z.hg + r]
                        total = v if total is None else jnp.where(group == j, v, total)
                    field[a * z.cx + q * z.xq + xq + 1, r] = rolled(total, -q * z.cy)
            total = None
            for j, (h, b) in enumerate(picks):
                v = rolled(every[a * z.n_ty + b, z.t_rows], h * z.n_ty * z.cy)
                total = v if total is None else jnp.where(group == j, v, total)
            total = rolled(total, -q * z.cy)
            for xq in range(z.xq):
                rate_ref[a * z.cx + q * z.xq + xq] = jnp.broadcast_to(
                    total[xq : xq + 1], (SUB, LANES)
                )

    src, dst = sweeps(z, field, other, rate_ref)
    blocks, _ = swap_blocks(z, src, dst)

    first_half = lane_ids((z.rows // 2, LANES)) < z.block
    pitch = z.rows + PITCH_PAD

    def fine_block(f, carry):
        v = blocks[z.block_place(blocks_ref[f]) + 1].reshape(z.rows // 2, LANES)
        turned = rolled(v, z.block)
        hi, turned_hi = v.astype(jnp.bfloat16), turned.astype(jnp.bfloat16)
        hi32, turned32 = hi.astype(jnp.float32), turned_hi.astype(jnp.float32)
        upper = jnp.where(first_half, hi32, turned - turned32).astype(jnp.bfloat16)
        lower = jnp.where(first_half, turned32, v - hi32).astype(jnp.bfloat16)
        lhs = jnp.concatenate(
            [
                jnp.concatenate([upper, lower], axis=0),
                jnp.concatenate([hi[:, : z.block], turned_hi[:, : z.block]], axis=0),
            ],
            axis=1,
        )
        out = jnp.dot(lhs, w_ref[f], preferred_element_type=jnp.float32)
        start = pl.multiple_of(f * pitch, SUB)
        for t in range(z.ct):
            fine_ref[t, pl.ds(start, z.rows), :] = out[:, t * LANES : (t + 1) * LANES]
        return carry

    lax.fori_loop(0, z.fine, fine_block, 0, unroll=16)

    def level(l, carry):
        for t in range(z.ct):
            cols = slice(t * LANES, (t + 1) * LANES)
            fine = [
                fine_ref[t, pl.ds(m * z.levels + l, z.fine, stride=pitch), :]
                for m in range(z.members)
            ]
            for v in range(z.vars):
                total = None
                for m in range(z.members):
                    term = fine[m] * pert_ref[m, l, v, :, cols].astype(jnp.float32)
                    total = term if total is None else total + term
                inc[l * z.vars + v, :, cols] = total
        return carry

    lax.fori_loop(0, z.levels, level, 0)

    where, _ = split2(cells_ref[...], z.bcells)
    ids = lax.broadcasted_iota(jnp.int32, (z.fine, z.obs), 0)
    here = ids == where
    for l in range(z.levels):
        part = inc[l * z.vars : (l + 1) * z.vars].reshape(z.vars * z.fine, z.bcells)
        hi, lo = hi_lo(part)
        seen = jnp.dot(hi, column_ref[...], preferred_element_type=jnp.float32) + jnp.dot(
            lo, column_ref[...], preferred_element_type=jnp.float32
        )
        for v in range(z.vars):
            s = l * z.vars + v
            got = jnp.where(here, seen[v * z.fine : (v + 1) * z.fine], 0.0)
            seen_ref[s : s + 1, : z.obs] = jnp.sum(got, axis=0, keepdims=True)
    seen_ref[:, z.obs :] = jnp.zeros((z.slabs, LANES), jnp.float32)
    for g in range(z.n_mem):
        mine = slice(g * z.slab_dev, (g + 1) * z.slab_dev)
        seen_ref[mine, : z.obs] -= jnp.where(g == me, dep_ref[...], 0.0)
    for j in range(z.slab_dev):
        for t in range(z.ot):
            at = j * z.ot + t
            seen_ref[at : at + 1, z.obs :] = ow_ref[j : j + 1, t * LANES : (t + 1) * LANES]
    for s in range(z.n_mem):
        to = lax.rem(me + s, z.n_mem)
        for j in range(z.slab_dev):
            inc_refs[s][j] = inc[to * z.slab_dev + j]


def adjoint_kernel(z, *refs):
    blocks_ref, used_ref = refs[:2]
    seen_refs = refs[2 : 2 + z.n_mem]
    w_ref, pert_ref, cells_ref, column_ref, rate_ref = refs[2 + z.n_mem : 7 + z.n_mem]
    out_ref, keep_ref, send_ref = refs[7 + z.n_mem : 10 + z.n_mem]
    every, field, other, fine_ref, force, obs_w = refs[10 + z.n_mem :]
    me = lax.axis_index("mem")
    total = None
    for s in range(z.n_mem):
        part = seen_refs[s][:, : z.obs]
        total = part if total is None else total + part
        obs_w[lax.rem(me + (z.n_mem - s), z.n_mem)] = seen_refs[s][:, z.obs :]
    used = used_ref[...] > 0.5
    where, _ = split2(cells_ref[...], z.bcells)
    ids = lax.broadcasted_iota(jnp.int32, (z.fine, z.obs), 0)
    here = ids == where
    rows = []
    for s in range(z.slabs):
        g, j = divmod(s, z.slab_dev)
        w = jnp.concatenate([obs_w[g, j * z.ot + t : j * z.ot + t + 1] for t in range(z.ot)], axis=1)
        rows.append(jnp.where(used, w * total[s : s + 1], 0.0))
    for j in range(z.slab_dev):
        mine = rows[j]
        for g in range(1, z.n_mem):
            mine = jnp.where(g == me, rows[g * z.slab_dev + j], mine)
        out_ref[j : j + 1] = mine
    dims = (((1,), (1,)), ((), ()))
    for l in range(z.levels):
        his, los = [], []
        for v in range(z.vars):
            row = jnp.where(here, rows[l * z.vars + v], 0.0)
            hi, lo = hi_lo(row)
            his.append(hi)
            los.append(lo)
        part = lax.dot_general(
            jnp.concatenate(his, axis=0), column_ref[...], dims, preferred_element_type=jnp.float32
        ) + lax.dot_general(
            jnp.concatenate(los, axis=0), column_ref[...], dims, preferred_element_type=jnp.float32
        )
        force[l * z.vars : (l + 1) * z.vars] = part.reshape(z.vars, z.fine, z.bcells)

    pitch = z.fine + PITCH_PAD

    def level(l, carry):
        for t in range(z.ct):
            cols = slice(t * LANES, (t + 1) * LANES)
            f = [force[l * z.vars + v, :, cols] for v in range(z.vars)]
            for m in range(z.members):
                grad = None
                for v in range(z.vars):
                    term = f[v] * pert_ref[m, l, v, :, cols].astype(jnp.float32)
                    grad = term if grad is None else grad + term
                start = pl.multiple_of((m * z.levels + l) * pitch, SUB)
                fine_ref[t, pl.ds(start, z.fine), :] = grad
        return carry

    lax.fori_loop(0, z.levels, level, 0)
    other[...] = jnp.zeros(other.shape, jnp.float32)
    first_half = lane_ids((z.rows // 2, LANES)) < z.block

    def fine_block(f, carry):
        at = z.block_place(blocks_ref[f]) + 1
        grad = jnp.concatenate(
            [fine_ref[t, pl.ds(f, z.rows, stride=pitch), :] for t in range(z.ct)], axis=1
        )
        hi, lo = hi_lo(grad)
        out = lax.dot_general(
            jnp.concatenate([hi, lo], axis=0),
            w_ref[f, z.block :, :],
            dims,
            preferred_element_type=jnp.float32,
        )
        out = out[: z.rows] + out[z.rows :]
        upper, lower = out[: z.rows // 2], out[z.rows // 2 :]
        out = jnp.where(first_half, upper, lower)
        out = out + rolled(jnp.where(first_half, lower, upper), z.block)
        other[at] += out.reshape(z.hg, SUB, LANES)
        return carry

    lax.fori_loop(0, z.fine, fine_block, 0, unroll=16)
    swap_blocks(z, other, field, rate_ref)
    clear_edges(z, field)
    clear_edges(z, other)
    grid, _ = sweeps(z, field, other, rate_ref)

    group = lane_ids((SUB, LANES)) // z.cy
    for a in range(z.n_tx):
        for xq in range(z.xq):
            turned = []
            for q in range(z.nq):
                x = a * z.cx + q * z.xq + xq
                inverse = 1.0 / rate_ref[x]
                turned.append([rolled(grid[x + 1, r] * inverse, q * z.cy) for r in range(z.hg)])
            for b in range(z.n_ty):
                for h in range(z.halves):
                    for r in range(z.hg):
                        total = turned[-(h * z.n_ty + b) % z.nq][r]
                        for j in range(1, z.nq):
                            v = turned[(j - h * z.n_ty - b) % z.nq][r]
                            total = jnp.where(group == j, v, total)
                        every[a * z.n_ty + b, xq * z.rg + h * z.hg + r] = total
    for s in range(z.chips):
        keep_ref[s] = every[z.tile_at(s, False, False)]
        send_ref[s] = every[z.tile_at(s, False, True)]


def finish_kernel(z, alpha_ref, *refs):
    out_ref = refs[-1]
    total = refs[0][...]
    for ref in refs[1:-1]:
        total = total + ref[...]
    b = lax.axis_index("ty")
    for xq in range(z.xq):
        rows = []
        for g in range(z.rg):
            turn = lax.rem(LANES - (g // z.hg * z.n_ty + b) * z.cy, LANES)
            rows.append(pltpu.roll(total[xq * z.rg + g], turn, 1))
        part = jnp.concatenate(rows, axis=0)
        for q in range(z.nq):
            x = q * z.xq + xq
            out_ref[:, x, :] = alpha_ref[:, x, :] + part[:, q * z.cy : (q + 1) * z.cy]


def on_device(
    alpha,
    filter_rate,
    block_list,
    interp_weights,
    perturbations,
    obs_cells,
    obs_count,
    departures,
    obs_weight,
):
    z = Sizes(alpha, interp_weights, perturbations, obs_cells, departures)
    f32, bf16 = jnp.float32, jnp.bfloat16
    shape = jax.ShapeDtypeStruct
    coarse = alpha.reshape(z.rows, z.cx, z.cy)
    wanted = block_list.reshape(z.fine)
    weights = interp_weights.reshape(z.fine, z.block, z.bcells)
    cells = obs_cells.reshape(1, z.obs)
    dep = departures.reshape(z.slab_dev, z.obs)
    ow = obs_weight.reshape(z.slab_dev, z.obs)
    axes = ("tx", "ty")
    tile_shape = (z.t_rows, SUB, LANES)
    full_shape = (z.t_rows + 1, SUB, LANES)
    grid_shape = (z.nx + 2, z.hg, SUB, LANES)

    own = pl.pallas_call(
        functools.partial(pack_kernel, z),
        out_shape=shape(full_shape, f32),
        in_specs=[HB, HB],
        out_specs=VM,
        scratch_shapes=[
            pltpu.VMEM(coarse.shape, f32),
            pltpu.VMEM(filter_rate.shape, f32),
            pltpu.SemaphoreType.DMA((2,)),
        ],
        compiler_params=params(8),
        name="pack",
    )(in_hbm(coarse), in_hbm(filter_rate))
    tiles = [own]
    for s in range(1, z.chips):
        tiles.append(lax.ppermute(own, axes, z.chip_perm(s)))
    for s in range(z.chips):
        tiles.append(lax.ppermute(tiles[s], axes, z.core_perm()))

    stacked, column, used = pl.pallas_call(
        functools.partial(prep_kernel, z),
        out_shape=(
            shape((z.fine, 3 * z.block, z.bcells), bf16),
            shape((z.bcells, z.obs), bf16),
            shape((1, z.obs), f32),
        ),
        in_specs=[HB, HB, SM],
        out_specs=(VM, VM, VM),
        scratch_shapes=[
            pltpu.VMEM(weights.shape, f32),
            pltpu.VMEM(cells.shape, jnp.int32),
            pltpu.SemaphoreType.DMA((PREP_CHUNKS + 1,)),
        ],
        compiler_params=params(16),
        cost_estimate=pl.CostEstimate(flops=4_000_000, bytes_accessed=5_000_000, transcendentals=0),
        name="prep",
    )(in_hbm(weights), in_hbm(cells), obs_count)

    pitch = z.rows + PITCH_PAD
    slab_shape = (z.slab_dev, z.fine, z.bcells)
    outs = pl.pallas_call(
        functools.partial(forward_kernel, z),
        out_shape=(
            shape((z.slabs, z.obs + LANES), f32),
            shape((z.nx, SUB, LANES), f32),
            *[shape(slab_shape, f32)] * z.n_mem,
        ),
        in_specs=[SM] + [VM] * (z.tiles + 6),
        out_specs=(VM,) * (2 + z.n_mem),
        scratch_shapes=[
            pltpu.VMEM((z.tiles, *full_shape), f32),
            pltpu.VMEM(grid_shape, f32),
            pltpu.VMEM(grid_shape, f32),
            pltpu.VMEM((z.ct, z.fine * pitch, LANES), f32),
            pltpu.VMEM((z.slabs, z.fine, z.bcells), f32),
        ],
        compiler_params=params(24),
        cost_estimate=pl.CostEstimate(flops=20_000_000, bytes_accessed=8_000_000, transcendentals=0),
        name="forward",
    )(wanted, *tiles, stacked, perturbations, cells, column, dep, ow)
    seen, rate, incs = outs[0], outs[1], outs[2:]

    def ring(step):
        return [(i, (i + step) % z.n_mem) for i in range(z.n_mem)]

    steps = range(1, z.n_mem)
    seens, parts = [seen], []
    for s in steps:
        seens.append(lax.ppermute(seen, "mem", ring(s)))
    for s in steps:
        parts.append(lax.ppermute(incs[s], "mem", ring(s)))

    pitch = z.fine + PITCH_PAD
    weighted, keep, send = pl.pallas_call(
        functools.partial(adjoint_kernel, z),
        out_shape=(
            shape((z.slab_dev, z.obs), f32),
            shape((z.chips, *tile_shape), f32),
            shape((z.chips, *tile_shape), f32),
        ),
        in_specs=[SM] + [VM] * (z.n_mem + 6),
        out_specs=(VM, VM, VM),
        scratch_shapes=[
            pltpu.VMEM((z.tiles, *tile_shape), f32),
            pltpu.VMEM(grid_shape, f32),
            pltpu.VMEM(grid_shape, f32),
            pltpu.VMEM((z.ct, z.rows * pitch, LANES), f32),
            pltpu.VMEM((z.slabs, z.fine, z.bcells), f32),
            pltpu.VMEM((z.n_mem, z.slabs, LANES), f32),
        ],
        compiler_params=params(24),
        cost_estimate=pl.CostEstimate(flops=20_000_000, bytes_accessed=8_000_000, transcendentals=0),
        name="adjoint",
    )(wanted, used, *seens, stacked, perturbations, cells, column, rate)

    came = lax.ppermute(send, axes, z.core_perm())
    sums = [keep[s] + came[s] for s in range(z.chips)]
    sums = [sums[0]] + [lax.ppermute(sums[s], axes, z.chip_perm(s)) for s in range(1, z.chips)]
    gradient = pl.pallas_call(
        functools.partial(finish_kernel, z),
        out_shape=shape((z.rows, z.cx, z.cy), f32),
        in_specs=[VM] * (1 + z.chips),
        out_specs=VM,
        compiler_params=params(8),
        name="finish",
    )(coarse, *sums)
    increment = incs[0]
    for part in parts:
        increment = increment + part
    return (increment, weighted.reshape(departures.shape), gradient.reshape(alpha.shape))


def solution(mesh):
    return jax.shard_map(
        on_device,
        mesh=mesh,
        in_specs=(
            P("mem", None, "tx", "ty"),
            P("tx", "ty"),
            P("tx", "ty", None),
            P("tx", "ty", None, None, None),
            P("mem", None, None, ("tx", "ty"), None),
            P("tx", "ty", None),
            P("tx", "ty"),
            P("tx", "ty", "mem", None),
            P("tx", "ty", "mem", None),
        ),
        out_specs=(
            P("mem", ("tx", "ty"), None),
            P("tx", "ty", "mem", None),
            P("mem", None, "tx", "ty"),
        ),
        check_vma=False,
    )
```

```python
import functools

import jax
import jax.numpy as jnp
from jax import lax
from jax.experimental import pallas as pl
from jax.experimental.pallas import tpu as pltpu
from jax.sharding import PartitionSpec as P


CB = 8
SWEEPS = 4
LANES = 128
SUB = 8
PITCH_PAD = 8
PREP_CHUNKS = 4
SWAP_UNROLL = 16


VM = pl.BlockSpec(memory_space=pltpu.VMEM)
HB = pl.BlockSpec(memory_space=pltpu.HBM)
SM = pl.BlockSpec(memory_space=pltpu.SMEM)


def in_hbm(v):
    return pltpu.with_memory_space_constraint(v, pltpu.HBM)


def params(mib):
    return pltpu.CompilerParams(vmem_limit_bytes=mib << 20)


def split2(v, n):
    if n & (n - 1) == 0:
        return v >> (n.bit_length() - 1), v & (n - 1)
    return lax.div(v, n), lax.rem(v, n)


def hi_lo(v):
    hi = v.astype(jnp.bfloat16)
    return hi, (v - hi.astype(jnp.float32)).astype(jnp.bfloat16)


def lane_ids(shape):
    return lax.broadcasted_iota(jnp.int32, shape, len(shape) - 1)


class Sizes:
    def __init__(self, alpha, weights, perts, cells, departures):
        self.n_tx, self.n_ty, self.n_mem = (lax.axis_size(a) for a in ("tx", "ty", "mem"))
        self.tiles = self.n_tx * self.n_ty
        self.chips = self.tiles // 2
        self.members, self.levels, self.cx, self.cy = alpha.shape
        self.rows = self.members * self.levels
        self.rg = self.rows // SUB
        self.fine, self.block, self.bcells = weights.shape[2:]
        self.vars = perts.shape[2]
        self.slabs = self.levels * self.vars
        self.slab_dev = departures.shape[2]
        self.obs = cells.shape[-1]
        self.nx, self.ny = self.n_tx * self.cx, self.n_ty * self.cy
        self.halves = LANES // self.ny
        self.hg = self.rg // self.halves
        self.nq = LANES // self.cy
        self.xq = self.cx // self.nq
        self.t_rows = self.xq * self.rg
        self.ct = self.bcells // LANES
        self.ot = self.obs // LANES
        self.blk_x, self.blk_y = self.cx // CB, self.cy // CB
        assert self.n_tx % 2 == 0 and self.halves * self.ny == LANES and self.ny == CB * CB
        assert self.nq * self.cy == LANES and self.xq * self.nq == self.cx and self.xq <= SUB
        assert self.halves == 2 and self.hg * 2 * SUB == self.rows
        assert self.nq == self.halves * self.n_ty
        assert self.slab_dev * self.ot <= self.slabs

    def block_place(self, bid):
        tile, kb = split2(bid, self.blk_x * self.blk_y)
        a, b = split2(tile, self.n_ty)
        bx, by = split2(kb, self.blk_y)
        return (a * self.blk_x + bx) * CB + b * self.blk_y + by

    def tile_at(self, step, back, other_core):
        tx, ty = lax.axis_index("tx"), lax.axis_index("ty")
        half = self.n_tx // 2
        chip_y, core = split2(tx, 2)
        dy, dx = divmod(step, self.n_ty)
        if back:
            dy, dx = half - dy, self.n_ty - dx
        y = lax.rem(chip_y + dy, half)
        x = lax.rem(ty + dx, self.n_ty)
        if other_core:
            core = 1 - core
        return (y * 2 + core) * self.n_ty + x

    def chip_perm(self, step):
        half = self.n_tx // 2
        dy, dx = divmod(step, self.n_ty)
        pairs = []
        for y in range(half):
            for core in range(2):
                for x in range(self.n_ty):
                    to = ((y + dy) % half * 2 + core) * self.n_ty + (x + dx) % self.n_ty
                    pairs.append(((y * 2 + core) * self.n_ty + x, to))
        return pairs

    def core_perm(self):
        return [(i, (i // self.n_ty ^ 1) * self.n_ty + i % self.n_ty) for i in range(self.tiles)]


def rolled(v, shift):
    shift %= LANES
    return v if shift == 0 else pltpu.roll(v, shift, v.ndim - 1)


def pack_kernel(z, alpha_hbm, rate_hbm, out_ref, alpha_ref, rate_ref, sems):
    copies = [
        pltpu.make_async_copy(alpha_hbm, alpha_ref, sems.at[0]),
        pltpu.make_async_copy(rate_hbm, rate_ref, sems.at[1]),
    ]
    for copy in copies:
        copy.start()
    for copy in copies:
        copy.wait()
    rate_rows, tiles = [], []
    for xq in range(z.xq):
        parts = [alpha_ref[:, q * z.xq + xq, :] for q in range(z.nq)]
        tiles.append(jnp.concatenate(parts, axis=1).reshape(z.rg, SUB, LANES))
        parts = [rate_ref[q * z.xq + xq : q * z.xq + xq + 1, :] for q in range(z.nq)]
        rate_rows.append(jnp.concatenate(parts, axis=1))
    b = lax.axis_index("ty")
    for xq in range(z.xq):
        for g in range(z.rg):
            turn = (g // z.hg * z.n_ty + b) * z.cy
            out_ref[xq * z.rg + g] = pltpu.roll(tiles[xq][g], turn, 1)
    rate_rows += [jnp.zeros((SUB - z.xq, LANES), jnp.float32)]
    out_ref[z.t_rows] = pltpu.roll(jnp.concatenate(rate_rows, axis=0), b * z.cy, 1)


def prep_kernel(z, *refs):
    weights_hbm, cells_hbm, count_ref, stacked_ref, column_ref, used_ref = refs[:6]
    weights_ref, cells_ref, sems = refs[6:]
    k = z.block
    chunk = z.fine // PREP_CHUNKS
    copies = []
    for i in range(PREP_CHUNKS):
        part = pl.ds(i * chunk, chunk)
        copies.append(
            pltpu.make_async_copy(weights_hbm.at[part], weights_ref.at[part], sems.at[i])
        )
    cells_copy = pltpu.make_async_copy(cells_hbm, cells_ref, sems.at[PREP_CHUNKS])
    for copy in [cells_copy] + copies:
        copy.start()
    used_ref[...] = jnp.where(lane_ids((1, z.obs)) < count_ref[0, 0], 1.0, 0.0)
    cells_copy.wait()
    _, col = split2(cells_ref[...], z.bcells)
    ids = lax.broadcasted_iota(jnp.int32, (z.bcells, z.obs), 0)
    column_ref[...] = jnp.where(ids == col, 1.0, 0.0).astype(jnp.bfloat16)

    def one(f, carry):
        hi, lo = hi_lo(weights_ref[f])
        stacked_ref[f, 0:k, :] = hi
        stacked_ref[f, k : 2 * k, :] = lo
        return carry

    for i in range(PREP_CHUNKS):
        copies[i].wait()
        lax.fori_loop(i * chunk, (i + 1) * chunk, one, 0, unroll=2)


def clear_edges(z, ref):
    for x in (0, z.nx + 1):
        ref[x] = jnp.zeros((z.hg, SUB, LANES), jnp.float32)


def sweeps(z, src, dst, rate_ref):
    lane_y = lane_ids((z.hg, SUB, LANES)) % z.ny
    for _ in range(SWEEPS):

        def row(x, carry, src=src, dst=dst):
            c = src[x + 1]
            west = jnp.where(lane_y > 0, rolled(c, 1), 0.0)
            east = jnp.where(lane_y < z.ny - 1, rolled(c, -1), 0.0)
            near = (src[x] + src[x + 2]) + (west + east)
            dst[x + 1] = c + rate_ref[x] * (near - 4.0 * c)
            return carry

        lax.fori_loop(0, z.nx, row, 0, unroll=True)
        src, dst = dst, src
    return src, dst


def swap_blocks(z, src, dst, rate_ref=None):
    lane = lane_ids((SUB, LANES))
    for bit in (1, 2, 4):
        shift = bit * CB
        low = (lane & shift) == 0

        def one(i, carry, src=src, dst=dst):
            bx, r = split2(i, z.hg)
            for j in range(CB):
                if j & bit == 0:
                    at, to = bx * CB + j, bx * CB + (j | bit)
                    a, b = src[at + 1, r], src[to + 1, r]
                    first = jnp.where(low, a, rolled(b, shift))
                    second = jnp.where(low, rolled(a, -shift), b)
                    if rate_ref is not None and bit == 4:
                        first, second = first * rate_ref[at], second * rate_ref[to]
                    dst[at + 1, r] = first
                    dst[to + 1, r] = second
            return carry

        lax.fori_loop(0, z.nx // CB * z.hg, one, 0, unroll=SWAP_UNROLL)
        src, dst = dst, src
    return src, dst


def forward_kernel(z, *refs):
    blocks_ref = refs[0]
    tile_refs = refs[1 : 1 + z.tiles]
    w_ref, pert_ref, cells_ref, column_ref, dep_ref, ow_ref = refs[1 + z.tiles : 7 + z.tiles]
    outs = refs[7 + z.tiles :]
    seen_ref, rate_ref = outs[:2]
    inc_refs = outs[2 : 2 + z.n_mem]
    every, field, other, fine_ref, inc = outs[2 + z.n_mem :]
    me = lax.axis_index("mem")
    for s in range(z.chips):
        every[z.tile_at(s, True, False)] = tile_refs[s][...]
        every[z.tile_at(s, True, True)] = tile_refs[z.chips + s][...]

    clear_edges(z, field)
    clear_edges(z, other)
    group = lane_ids((SUB, LANES)) // z.cy
    for a in range(z.n_tx):
        for q in range(z.nq):
            picks = [divmod((j - q) % z.nq, z.n_ty) for j in range(z.nq)]
            for xq in range(z.xq):
                for r in range(z.hg):
                    total = None
                    for j, (h, b) in enumerate(picks):
                        v = every[a * z.n_ty + b, xq * z.rg + h * z.hg + r]
                        total = v if total is None else jnp.where(group == j, v, total)
                    field[a * z.cx + q * z.xq + xq + 1, r] = rolled(total, -q * z.cy)
            total = None
            for j, (h, b) in enumerate(picks):
                v = rolled(every[a * z.n_ty + b, z.t_rows], h * z.n_ty * z.cy)
                total = v if total is None else jnp.where(group == j, v, total)
            total = rolled(total, -q * z.cy)
            for xq in range(z.xq):
                rate_ref[a * z.cx + q * z.xq + xq] = jnp.broadcast_to(
                    total[xq : xq + 1], (SUB, LANES)
                )

    src, dst = sweeps(z, field, other, rate_ref)
    blocks, _ = swap_blocks(z, src, dst)

    first_half = lane_ids((z.rows // 2, LANES)) < z.block
    low_lanes = lane_ids((z.rows, LANES)) < z.block
    pitch = z.rows + PITCH_PAD

    def fine_block(f, carry):
        v = blocks[z.block_place(blocks_ref[f]) + 1].reshape(z.rows // 2, LANES)
        turned = rolled(v, z.block)
        v = jnp.concatenate(
            [jnp.where(first_half, v, turned), jnp.where(first_half, turned, v)], axis=0
        )
        hi = v.astype(jnp.bfloat16)
        lo = jnp.where(low_lanes, v - hi.astype(jnp.float32), 0.0).astype(jnp.bfloat16)
        lhs = jnp.concatenate([hi, lo], axis=0)
        out = jnp.dot(lhs, w_ref[f], preferred_element_type=jnp.float32)
        out = out[: z.rows] + out[z.rows :]
        start = pl.multiple_of(f * pitch, SUB)
        for t in range(z.ct):
            fine_ref[t, pl.ds(start, z.rows), :] = out[:, t * LANES : (t + 1) * LANES]
        return carry

    lax.fori_loop(0, z.fine, fine_block, 0, unroll=16)

    def level(l, carry):
        for t in range(z.ct):
            cols = slice(t * LANES, (t + 1) * LANES)
            fine = [
                fine_ref[t, pl.ds(m * z.levels + l, z.fine, stride=pitch), :]
                for m in range(z.members)
            ]
            for v in range(z.vars):
                total = None
                for m in range(z.members):
                    term = fine[m] * pert_ref[m, l, v, :, cols].astype(jnp.float32)
                    total = term if total is None else total + term
                inc[l * z.vars + v, :, cols] = total
        return carry

    lax.fori_loop(0, z.levels, level, 0)

    where, _ = split2(cells_ref[...], z.bcells)
    ids = lax.broadcasted_iota(jnp.int32, (z.fine, z.obs), 0)
    here = ids == where
    for l in range(z.levels):
        part = inc[l * z.vars : (l + 1) * z.vars].reshape(z.vars * z.fine, z.bcells)
        hi, lo = hi_lo(part)
        seen = jnp.dot(hi, column_ref[...], preferred_element_type=jnp.float32) + jnp.dot(
            lo, column_ref[...], preferred_element_type=jnp.float32
        )
        for v in range(z.vars):
            s = l * z.vars + v
            got = jnp.where(here, seen[v * z.fine : (v + 1) * z.fine], 0.0)
            seen_ref[s : s + 1, : z.obs] = jnp.sum(got, axis=0, keepdims=True)
    seen_ref[:, z.obs :] = jnp.zeros((z.slabs, LANES), jnp.float32)
    for g in range(z.n_mem):
        mine = slice(g * z.slab_dev, (g + 1) * z.slab_dev)
        seen_ref[mine, : z.obs] -= jnp.where(g == me, dep_ref[...], 0.0)
    for j in range(z.slab_dev):
        for t in range(z.ot):
            at = j * z.ot + t
            seen_ref[at : at + 1, z.obs :] = ow_ref[j : j + 1, t * LANES : (t + 1) * LANES]
    for s in range(z.n_mem):
        to = lax.rem(me + s, z.n_mem)
        for j in range(z.slab_dev):
            inc_refs[s][j] = inc[to * z.slab_dev + j]


def adjoint_kernel(z, *refs):
    blocks_ref, used_ref = refs[:2]
    seen_refs = refs[2 : 2 + z.n_mem]
    w_ref, pert_ref, cells_ref, column_ref, rate_ref = refs[2 + z.n_mem : 7 + z.n_mem]
    out_ref, keep_ref, send_ref = refs[7 + z.n_mem : 10 + z.n_mem]
    every, field, other, fine_ref, force, obs_w = refs[10 + z.n_mem :]
    me = lax.axis_index("mem")
    total = None
    for s in range(z.n_mem):
        part = seen_refs[s][:, : z.obs]
        total = part if total is None else total + part
        obs_w[lax.rem(me + (z.n_mem - s), z.n_mem)] = seen_refs[s][:, z.obs :]
    used = used_ref[...] > 0.5
    where, _ = split2(cells_ref[...], z.bcells)
    ids = lax.broadcasted_iota(jnp.int32, (z.fine, z.obs), 0)
    here = ids == where
    rows = []
    for s in range(z.slabs):
        g, j = divmod(s, z.slab_dev)
        w = jnp.concatenate([obs_w[g, j * z.ot + t : j * z.ot + t + 1] for t in range(z.ot)], axis=1)
        rows.append(jnp.where(used, w * total[s : s + 1], 0.0))
    for j in range(z.slab_dev):
        mine = rows[j]
        for g in range(1, z.n_mem):
            mine = jnp.where(g == me, rows[g * z.slab_dev + j], mine)
        out_ref[j : j + 1] = mine
    dims = (((1,), (1,)), ((), ()))
    for l in range(z.levels):
        his, los = [], []
        for v in range(z.vars):
            row = jnp.where(here, rows[l * z.vars + v], 0.0)
            hi, lo = hi_lo(row)
            his.append(hi)
            los.append(lo)
        part = lax.dot_general(
            jnp.concatenate(his, axis=0), column_ref[...], dims, preferred_element_type=jnp.float32
        ) + lax.dot_general(
            jnp.concatenate(los, axis=0), column_ref[...], dims, preferred_element_type=jnp.float32
        )
        force[l * z.vars : (l + 1) * z.vars] = part.reshape(z.vars, z.fine, z.bcells)

    pitch = z.fine + PITCH_PAD

    def level(l, carry):
        for t in range(z.ct):
            cols = slice(t * LANES, (t + 1) * LANES)
            f = [force[l * z.vars + v, :, cols] for v in range(z.vars)]
            for m in range(z.members):
                grad = None
                for v in range(z.vars):
                    term = f[v] * pert_ref[m, l, v, :, cols].astype(jnp.float32)
                    grad = term if grad is None else grad + term
                start = pl.multiple_of((m * z.levels + l) * pitch, SUB)
                fine_ref[t, pl.ds(start, z.fine), :] = grad
        return carry

    lax.fori_loop(0, z.levels, level, 0)
    other[...] = jnp.zeros(other.shape, jnp.float32)
    first_half = lane_ids((z.rows // 2, LANES)) < z.block

    def fine_block(f, carry):
        at = z.block_place(blocks_ref[f]) + 1
        grad = jnp.concatenate(
            [fine_ref[t, pl.ds(f, z.rows, stride=pitch), :] for t in range(z.ct)], axis=1
        )
        hi, lo = hi_lo(grad)
        out = lax.dot_general(
            jnp.concatenate([hi, lo], axis=0),
            w_ref[f],
            dims,
            preferred_element_type=jnp.float32,
        )
        out = out[: z.rows] + out[z.rows :]
        upper, lower = out[: z.rows // 2], out[z.rows // 2 :]
        out = jnp.where(first_half, upper, lower)
        out = out + rolled(jnp.where(first_half, lower, upper), z.block)
        other[at] += out.reshape(z.hg, SUB, LANES)
        return carry

    lax.fori_loop(0, z.fine, fine_block, 0, unroll=16)
    swap_blocks(z, other, field, rate_ref)
    clear_edges(z, field)
    clear_edges(z, other)
    grid, _ = sweeps(z, field, other, rate_ref)

    group = lane_ids((SUB, LANES)) // z.cy
    for a in range(z.n_tx):
        for xq in range(z.xq):
            turned = []
            for q in range(z.nq):
                x = a * z.cx + q * z.xq + xq
                inverse = 1.0 / rate_ref[x]
                turned.append([rolled(grid[x + 1, r] * inverse, q * z.cy) for r in range(z.hg)])
            for b in range(z.n_ty):
                for h in range(z.halves):
                    for r in range(z.hg):
                        total = turned[-(h * z.n_ty + b) % z.nq][r]
                        for j in range(1, z.nq):
                            v = turned[(j - h * z.n_ty - b) % z.nq][r]
                            total = jnp.where(group == j, v, total)
                        every[a * z.n_ty + b, xq * z.rg + h * z.hg + r] = total
    for s in range(z.chips):
        keep_ref[s] = every[z.tile_at(s, False, False)]
        send_ref[s] = every[z.tile_at(s, False, True)]


def finish_kernel(z, alpha_ref, *refs):
    out_ref = refs[-1]
    total = refs[0][...]
    for ref in refs[1:-1]:
        total = total + ref[...]
    b = lax.axis_index("ty")
    for xq in range(z.xq):
        for g in range(z.rg):
            v = total[xq * z.rg + g]
            for q in range(z.nq):
                turn = lax.rem(2 * LANES - (q + g // z.hg * z.n_ty + b) * z.cy, LANES)
                rows = slice(g * SUB, (g + 1) * SUB)
                x = q * z.xq + xq
                out_ref[rows, x, :] = alpha_ref[rows, x, :] + pltpu.roll(v, turn, 1)[:, : z.cy]


def on_device(
    alpha,
    filter_rate,
    block_list,
    interp_weights,
    perturbations,
    obs_cells,
    obs_count,
    departures,
    obs_weight,
):
    z = Sizes(alpha, interp_weights, perturbations, obs_cells, departures)
    f32, bf16 = jnp.float32, jnp.bfloat16
    shape = jax.ShapeDtypeStruct
    coarse = alpha.reshape(z.rows, z.cx, z.cy)
    wanted = block_list.reshape(z.fine)
    weights = interp_weights.reshape(z.fine, z.block, z.bcells)
    cells = obs_cells.reshape(1, z.obs)
    dep = departures.reshape(z.slab_dev, z.obs)
    ow = obs_weight.reshape(z.slab_dev, z.obs)
    axes = ("tx", "ty")
    tile_shape = (z.t_rows, SUB, LANES)
    full_shape = (z.t_rows + 1, SUB, LANES)
    grid_shape = (z.nx + 2, z.hg, SUB, LANES)

    own = pl.pallas_call(
        functools.partial(pack_kernel, z),
        out_shape=shape(full_shape, f32),
        in_specs=[HB, HB],
        out_specs=VM,
        scratch_shapes=[
            pltpu.VMEM(coarse.shape, f32),
            pltpu.VMEM(filter_rate.shape, f32),
            pltpu.SemaphoreType.DMA((2,)),
        ],
        compiler_params=params(8),
        name="pack",
    )(in_hbm(coarse), in_hbm(filter_rate))
    tiles = [own]
    for s in range(1, z.chips):
        tiles.append(lax.ppermute(own, axes, z.chip_perm(s)))
    for s in range(z.chips):
        tiles.append(lax.ppermute(tiles[s], axes, z.core_perm()))

    stacked, column, used = pl.pallas_call(
        functools.partial(prep_kernel, z),
        out_shape=(
            shape((z.fine, 2 * z.block, z.bcells), bf16),
            shape((z.bcells, z.obs), bf16),
            shape((1, z.obs), f32),
        ),
        in_specs=[HB, HB, SM],
        out_specs=(VM, VM, VM),
        scratch_shapes=[
            pltpu.VMEM(weights.shape, f32),
            pltpu.VMEM(cells.shape, jnp.int32),
            pltpu.SemaphoreType.DMA((PREP_CHUNKS + 1,)),
        ],
        compiler_params=params(16),
        cost_estimate=pl.CostEstimate(flops=4_000_000, bytes_accessed=5_000_000, transcendentals=0),
        name="prep",
    )(in_hbm(weights), in_hbm(cells), obs_count)

    pitch = z.rows + PITCH_PAD
    slab_shape = (z.slab_dev, z.fine, z.bcells)
    outs = pl.pallas_call(
        functools.partial(forward_kernel, z),
        out_shape=(
            shape((z.slabs, z.obs + LANES), f32),
            shape((z.nx, SUB, LANES), f32),
            *[shape(slab_shape, f32)] * z.n_mem,
        ),
        in_specs=[SM] + [VM] * (z.tiles + 6),
        out_specs=(VM,) * (2 + z.n_mem),
        scratch_shapes=[
            pltpu.VMEM((z.tiles, *full_shape), f32),
            pltpu.VMEM(grid_shape, f32),
            pltpu.VMEM(grid_shape, f32),
            pltpu.VMEM((z.ct, z.fine * pitch, LANES), f32),
            pltpu.VMEM((z.slabs, z.fine, z.bcells), f32),
        ],
        compiler_params=params(24),
        cost_estimate=pl.CostEstimate(flops=20_000_000, bytes_accessed=8_000_000, transcendentals=0),
        name="forward",
    )(wanted, *tiles, stacked, perturbations, cells, column, dep, ow)
    seen, rate, incs = outs[0], outs[1], outs[2:]

    def ring(step):
        return [(i, (i + step) % z.n_mem) for i in range(z.n_mem)]

    steps = range(1, z.n_mem)
    seens, parts = [seen], []
    for s in steps:
        seens.append(lax.ppermute(seen, "mem", ring(s)))
    for s in steps:
        parts.append(lax.ppermute(incs[s], "mem", ring(s)))

    pitch = z.fine + PITCH_PAD
    weighted, keep, send = pl.pallas_call(
        functools.partial(adjoint_kernel, z),
        out_shape=(
            shape((z.slab_dev, z.obs), f32),
            shape((z.chips, *tile_shape), f32),
            shape((z.chips, *tile_shape), f32),
        ),
        in_specs=[SM] + [VM] * (z.n_mem + 6),
        out_specs=(VM, VM, VM),
        scratch_shapes=[
            pltpu.VMEM((z.tiles, *tile_shape), f32),
            pltpu.VMEM(grid_shape, f32),
            pltpu.VMEM(grid_shape, f32),
            pltpu.VMEM((z.ct, z.rows * pitch, LANES), f32),
            pltpu.VMEM((z.slabs, z.fine, z.bcells), f32),
            pltpu.VMEM((z.n_mem, z.slabs, LANES), f32),
        ],
        compiler_params=params(24),
        cost_estimate=pl.CostEstimate(flops=20_000_000, bytes_accessed=8_000_000, transcendentals=0),
        name="adjoint",
    )(wanted, used, *seens, stacked, perturbations, cells, column, rate)

    came = lax.ppermute(send, axes, z.core_perm())
    sums = [keep[s] + came[s] for s in range(z.chips)]
    sums = [sums[0]] + [lax.ppermute(sums[s], axes, z.chip_perm(s)) for s in range(1, z.chips)]
    gradient = pl.pallas_call(
        functools.partial(finish_kernel, z),
        out_shape=shape((z.rows, z.cx, z.cy), f32),
        in_specs=[VM] * (1 + z.chips),
        out_specs=VM,
        compiler_params=params(8),
        name="finish",
    )(coarse, *sums)
    increment = incs[0]
    for part in parts:
        increment = increment + part
    return (increment, weighted.reshape(departures.shape), gradient.reshape(alpha.shape))


def solution(mesh):
    return jax.shard_map(
        on_device,
        mesh=mesh,
        in_specs=(
            P("mem", None, "tx", "ty"),
            P("tx", "ty"),
            P("tx", "ty", None),
            P("tx", "ty", None, None, None),
            P("mem", None, None, ("tx", "ty"), None),
            P("tx", "ty", None),
            P("tx", "ty"),
            P("tx", "ty", "mem", None),
            P("tx", "ty", "mem", None),
        ),
        out_specs=(
            P("mem", ("tx", "ty"), None),
            P("tx", "ty", "mem", None),
            P("mem", None, "tx", "ty"),
        ),
        check_vma=False,
    )
```

```python
import functools

import jax
import jax.numpy as jnp
from jax import lax
from jax.experimental import pallas as pl
from jax.experimental.pallas import tpu as pltpu
from jax.sharding import PartitionSpec as P


CB = 8
SWEEPS = 4
LANES = 128
SUB = 8
PITCH_PAD = 8
PREP_CHUNKS = 4
SWAP_UNROLL = 16
PRODUCTS = 2


VM = pl.BlockSpec(memory_space=pltpu.VMEM)
HB = pl.BlockSpec(memory_space=pltpu.HBM)
SM = pl.BlockSpec(memory_space=pltpu.SMEM)


def in_hbm(v):
    return pltpu.with_memory_space_constraint(v, pltpu.HBM)


def params(mib):
    return pltpu.CompilerParams(vmem_limit_bytes=mib << 20)


def split2(v, n):
    if n & (n - 1) == 0:
        return v >> (n.bit_length() - 1), v & (n - 1)
    return lax.div(v, n), lax.rem(v, n)


def hi_lo(v):
    hi = v.astype(jnp.bfloat16)
    return hi, (v - hi.astype(jnp.float32)).astype(jnp.bfloat16)


def lane_ids(shape):
    return lax.broadcasted_iota(jnp.int32, shape, len(shape) - 1)


class Sizes:
    def __init__(self, alpha, weights, perts, cells, departures):
        self.n_tx, self.n_ty, self.n_mem = (lax.axis_size(a) for a in ("tx", "ty", "mem"))
        self.tiles = self.n_tx * self.n_ty
        self.chips = self.tiles // 2
        self.members, self.levels, self.cx, self.cy = alpha.shape
        self.rows = self.members * self.levels
        self.rg = self.rows // SUB
        self.fine, self.block, self.bcells = weights.shape[2:]
        self.vars = perts.shape[2]
        self.slabs = self.levels * self.vars
        self.slab_dev = departures.shape[2]
        self.obs = cells.shape[-1]
        self.nx, self.ny = self.n_tx * self.cx, self.n_ty * self.cy
        self.halves = LANES // self.ny
        self.hg = self.rg // self.halves
        self.nq = LANES // self.cy
        self.xq = self.cx // self.nq
        self.t_rows = self.xq * self.rg
        self.ct = self.bcells // LANES
        self.ot = self.obs // LANES
        self.blk_x, self.blk_y = self.cx // CB, self.cy // CB
        assert self.n_tx % 2 == 0 and self.halves * self.ny == LANES and self.ny == CB * CB
        assert self.nq * self.cy == LANES and self.xq * self.nq == self.cx and self.xq <= SUB
        assert self.halves == 2 and self.hg * 2 * SUB == self.rows
        assert self.nq == self.halves * self.n_ty
        assert self.slab_dev * self.ot <= self.slabs

    def block_place(self, bid):
        tile, kb = split2(bid, self.blk_x * self.blk_y)
        a, b = split2(tile, self.n_ty)
        bx, by = split2(kb, self.blk_y)
        return (a * self.blk_x + bx) * CB + b * self.blk_y + by

    def tile_at(self, step, back, other_core):
        tx, ty = lax.axis_index("tx"), lax.axis_index("ty")
        half = self.n_tx // 2
        chip_y, core = split2(tx, 2)
        dy, dx = divmod(step, self.n_ty)
        if back:
            dy, dx = half - dy, self.n_ty - dx
        y = lax.rem(chip_y + dy, half)
        x = lax.rem(ty + dx, self.n_ty)
        if other_core:
            core = 1 - core
        return (y * 2 + core) * self.n_ty + x

    def chip_perm(self, step):
        half = self.n_tx // 2
        dy, dx = divmod(step, self.n_ty)
        pairs = []
        for y in range(half):
            for core in range(2):
                for x in range(self.n_ty):
                    to = ((y + dy) % half * 2 + core) * self.n_ty + (x + dx) % self.n_ty
                    pairs.append(((y * 2 + core) * self.n_ty + x, to))
        return pairs

    def core_perm(self):
        return [(i, (i // self.n_ty ^ 1) * self.n_ty + i % self.n_ty) for i in range(self.tiles)]


def rolled(v, shift):
    shift %= LANES
    return v if shift == 0 else pltpu.roll(v, shift, v.ndim - 1)


def pack_kernel(z, alpha_hbm, rate_hbm, out_ref, alpha_ref, rate_ref, sems):
    copies = [
        pltpu.make_async_copy(alpha_hbm, alpha_ref, sems.at[0]),
        pltpu.make_async_copy(rate_hbm, rate_ref, sems.at[1]),
    ]
    for copy in copies:
        copy.start()
    for copy in copies:
        copy.wait()
    rate_rows, tiles = [], []
    for xq in range(z.xq):
        parts = [alpha_ref[:, q * z.xq + xq, :] for q in range(z.nq)]
        tiles.append(jnp.concatenate(parts, axis=1).reshape(z.rg, SUB, LANES))
        parts = [rate_ref[q * z.xq + xq : q * z.xq + xq + 1, :] for q in range(z.nq)]
        rate_rows.append(jnp.concatenate(parts, axis=1))
    b = lax.axis_index("ty")
    for xq in range(z.xq):
        for g in range(z.rg):
            turn = (g // z.hg * z.n_ty + b) * z.cy
            out_ref[xq * z.rg + g] = pltpu.roll(tiles[xq][g], turn, 1)
    rate_rows += [jnp.zeros((SUB - z.xq, LANES), jnp.float32)]
    out_ref[z.t_rows] = pltpu.roll(jnp.concatenate(rate_rows, axis=0), b * z.cy, 1)


def prep_kernel(z, *refs):
    weights_hbm, cells_hbm, count_ref, stacked_ref, column_ref, used_ref = refs[:6]
    weights_ref, cells_ref, sems = refs[6:]
    k = z.block
    chunk = z.fine // PREP_CHUNKS
    copies = []
    for i in range(PREP_CHUNKS):
        part = pl.ds(i * chunk, chunk)
        copies.append(
            pltpu.make_async_copy(weights_hbm.at[part], weights_ref.at[part], sems.at[i])
        )
    cells_copy = pltpu.make_async_copy(cells_hbm, cells_ref, sems.at[PREP_CHUNKS])
    for copy in [cells_copy] + copies:
        copy.start()
    used_ref[...] = jnp.where(lane_ids((1, z.obs)) < count_ref[0, 0], 1.0, 0.0)
    cells_copy.wait()
    _, col = split2(cells_ref[...], z.bcells)
    ids = lax.broadcasted_iota(jnp.int32, (z.bcells, z.obs), 0)
    column_ref[...] = jnp.where(ids == col, 1.0, 0.0).astype(jnp.bfloat16)

    def one(f, carry):
        hi, lo = hi_lo(weights_ref[f])
        stacked_ref[f, 0:k, :] = hi
        stacked_ref[f, k : 2 * k, :] = lo
        return carry

    for i in range(PREP_CHUNKS):
        copies[i].wait()
        lax.fori_loop(i * chunk, (i + 1) * chunk, one, 0, unroll=2)


def clear_edges(z, ref):
    for x in (0, z.nx + 1):
        ref[x] = jnp.zeros((z.hg, SUB, LANES), jnp.float32)


def sweeps(z, src, dst, rate_ref):
    lane_y = lane_ids((z.hg, SUB, LANES)) % z.ny
    for _ in range(SWEEPS):

        def row(x, carry, src=src, dst=dst):
            c = src[x + 1]
            west = jnp.where(lane_y > 0, rolled(c, 1), 0.0)
            east = jnp.where(lane_y < z.ny - 1, rolled(c, -1), 0.0)
            near = (src[x] + src[x + 2]) + (west + east)
            dst[x + 1] = c + rate_ref[x] * (near - 4.0 * c)
            return carry

        lax.fori_loop(0, z.nx, row, 0, unroll=True)
        src, dst = dst, src
    return src, dst


def swap_blocks(z, src, dst, rate_ref=None):
    lane = lane_ids((SUB, LANES))
    for bit in (1, 2, 4):
        shift = bit * CB
        low = (lane & shift) == 0

        def one(i, carry, src=src, dst=dst):
            bx, r = split2(i, z.hg)
            for j in range(CB):
                if j & bit == 0:
                    at, to = bx * CB + j, bx * CB + (j | bit)
                    a, b = src[at + 1, r], src[to + 1, r]
                    first = jnp.where(low, a, rolled(b, shift))
                    second = jnp.where(low, rolled(a, -shift), b)
                    if rate_ref is not None and bit == 4:
                        first, second = first * rate_ref[at], second * rate_ref[to]
                    dst[at + 1, r] = first
                    dst[to + 1, r] = second
            return carry

        lax.fori_loop(0, z.nx // CB * z.hg, one, 0, unroll=SWAP_UNROLL)
        src, dst = dst, src
    return src, dst


def forward_kernel(z, *refs):
    blocks_ref = refs[0]
    tile_refs = refs[1 : 1 + z.tiles]
    w_ref, pert_ref, cells_ref, column_ref, dep_ref, ow_ref = refs[1 + z.tiles : 7 + z.tiles]
    outs = refs[7 + z.tiles :]
    seen_ref, rate_ref = outs[:2]
    inc_refs = outs[2 : 2 + z.n_mem]
    every, field, other, fine_ref, inc = outs[2 + z.n_mem :]
    me = lax.axis_index("mem")
    for s in range(z.chips):
        every[z.tile_at(s, True, False)] = tile_refs[s][...]
        every[z.tile_at(s, True, True)] = tile_refs[z.chips + s][...]

    clear_edges(z, field)
    clear_edges(z, other)
    group = lane_ids((SUB, LANES)) // z.cy
    for a in range(z.n_tx):
        for q in range(z.nq):
            picks = [divmod((j - q) % z.nq, z.n_ty) for j in range(z.nq)]
            for xq in range(z.xq):
                for r in range(z.hg):
                    total = None
                    for j, (h, b) in enumerate(picks):
                        v = every[a * z.n_ty + b, xq * z.rg + h * z.hg + r]
                        total = v if total is None else jnp.where(group == j, v, total)
                    field[a * z.cx + q * z.xq + xq + 1, r] = rolled(total, -q * z.cy)
            total = None
            for j, (h, b) in enumerate(picks):
                v = rolled(every[a * z.n_ty + b, z.t_rows], h * z.n_ty * z.cy)
                total = v if total is None else jnp.where(group == j, v, total)
            total = rolled(total, -q * z.cy)
            for xq in range(z.xq):
                rate_ref[a * z.cx + q * z.xq + xq] = jnp.broadcast_to(
                    total[xq : xq + 1], (SUB, LANES)
                )

    src, dst = sweeps(z, field, other, rate_ref)
    blocks, _ = swap_blocks(z, src, dst)

    first_half = lane_ids((z.rows // 2, LANES)) < z.block
    low_lanes = lane_ids((z.rows, LANES)) < z.block
    pitch = z.rows + PITCH_PAD

    def fine_block(f, carry):
        v = blocks[z.block_place(blocks_ref[f]) + 1].reshape(z.rows // 2, LANES)
        turned = rolled(v, z.block)
        v = jnp.concatenate(
            [jnp.where(first_half, v, turned), jnp.where(first_half, turned, v)], axis=0
        )
        hi = v.astype(jnp.bfloat16)
        lo = jnp.where(low_lanes, v - hi.astype(jnp.float32), 0.0).astype(jnp.bfloat16)
        lhs = jnp.concatenate([hi, lo], axis=0)
        out = jnp.dot(lhs, w_ref[f], preferred_element_type=jnp.float32)
        out = out[: z.rows] + out[z.rows :]
        start = pl.multiple_of(f * pitch, SUB)
        for t in range(z.ct):
            fine_ref[t, pl.ds(start, z.rows), :] = out[:, t * LANES : (t + 1) * LANES]
        return carry

    lax.fori_loop(0, z.fine, fine_block, 0, unroll=16)

    def level(l, carry):
        for t in range(z.ct):
            cols = slice(t * LANES, (t + 1) * LANES)
            fine = [
                fine_ref[t, pl.ds(m * z.levels + l, z.fine, stride=pitch), :]
                for m in range(z.members)
            ]
            for v in range(z.vars):
                total = None
                for m in range(z.members):
                    term = fine[m] * pert_ref[m, l, v, :, cols].astype(jnp.float32)
                    total = term if total is None else total + term
                inc[l * z.vars + v, :, cols] = total
        return carry

    lax.fori_loop(0, z.levels, level, 0)

    where, _ = split2(cells_ref[...], z.bcells)
    ids = lax.broadcasted_iota(jnp.int32, (z.fine, z.obs), 0)
    here = ids == where
    n = z.slabs // PRODUCTS
    for i in range(PRODUCTS):
        hi, lo = hi_lo(inc[i * n : (i + 1) * n].reshape(n * z.fine, z.bcells))
        seen = jnp.dot(
            jnp.concatenate([hi, lo], axis=0), column_ref[...], preferred_element_type=jnp.float32
        )
        for k in range(n):
            part = seen[k * z.fine : (k + 1) * z.fine] + seen[(n + k) * z.fine : (n + k + 1) * z.fine]
            seen_ref[i * n + k : i * n + k + 1, : z.obs] = jnp.sum(
                jnp.where(here, part, 0.0), axis=0, keepdims=True
            )
    seen_ref[:, z.obs :] = jnp.zeros((z.slabs, LANES), jnp.float32)
    for g in range(z.n_mem):
        mine = slice(g * z.slab_dev, (g + 1) * z.slab_dev)
        seen_ref[mine, : z.obs] -= jnp.where(g == me, dep_ref[...], 0.0)
    for j in range(z.slab_dev):
        for t in range(z.ot):
            at = j * z.ot + t
            seen_ref[at : at + 1, z.obs :] = ow_ref[j : j + 1, t * LANES : (t + 1) * LANES]
    for s in range(z.n_mem):
        to = lax.rem(me + s, z.n_mem)
        for j in range(z.slab_dev):
            inc_refs[s][j] = inc[to * z.slab_dev + j]


def adjoint_kernel(z, *refs):
    blocks_ref, used_ref = refs[:2]
    seen_refs = refs[2 : 2 + z.n_mem]
    w_ref, pert_ref, cells_ref, column_ref, rate_ref = refs[2 + z.n_mem : 7 + z.n_mem]
    out_ref, keep_ref, send_ref = refs[7 + z.n_mem : 10 + z.n_mem]
    every, field, other, fine_ref, force, obs_w = refs[10 + z.n_mem :]
    me = lax.axis_index("mem")
    total = None
    for s in range(z.n_mem):
        part = seen_refs[s][:, : z.obs]
        total = part if total is None else total + part
        obs_w[lax.rem(me + (z.n_mem - s), z.n_mem)] = seen_refs[s][:, z.obs :]
    used = used_ref[...] > 0.5
    where, _ = split2(cells_ref[...], z.bcells)
    ids = lax.broadcasted_iota(jnp.int32, (z.fine, z.obs), 0)
    here = ids == where
    rows = []
    for s in range(z.slabs):
        g, j = divmod(s, z.slab_dev)
        w = jnp.concatenate([obs_w[g, j * z.ot + t : j * z.ot + t + 1] for t in range(z.ot)], axis=1)
        rows.append(jnp.where(used, w * total[s : s + 1], 0.0))
    for j in range(z.slab_dev):
        mine = rows[j]
        for g in range(1, z.n_mem):
            mine = jnp.where(g == me, rows[g * z.slab_dev + j], mine)
        out_ref[j : j + 1] = mine
    dims = (((1,), (1,)), ((), ()))
    n = z.slabs // PRODUCTS
    for i in range(PRODUCTS):
        his, los = [], []
        for k in range(n):
            hi, lo = hi_lo(rows[i * n + k])
            his.append(jnp.where(here, hi.astype(jnp.float32), 0.0).astype(jnp.bfloat16))
            los.append(jnp.where(here, lo.astype(jnp.float32), 0.0).astype(jnp.bfloat16))
        part = lax.dot_general(
            jnp.concatenate(his + los, axis=0),
            column_ref[...],
            dims,
            preferred_element_type=jnp.float32,
        )
        part = part[: n * z.fine] + part[n * z.fine :]
        force[i * n : (i + 1) * n] = part.reshape(n, z.fine, z.bcells)

    pitch = z.fine + PITCH_PAD

    def level(l, carry):
        for t in range(z.ct):
            cols = slice(t * LANES, (t + 1) * LANES)
            f = [force[l * z.vars + v, :, cols] for v in range(z.vars)]
            for m in range(z.members):
                grad = None
                for v in range(z.vars):
                    term = f[v] * pert_ref[m, l, v, :, cols].astype(jnp.float32)
                    grad = term if grad is None else grad + term
                start = pl.multiple_of((m * z.levels + l) * pitch, SUB)
                fine_ref[t, pl.ds(start, z.fine), :] = grad
        return carry

    lax.fori_loop(0, z.levels, level, 0)
    other[...] = jnp.zeros(other.shape, jnp.float32)
    first_half = lane_ids((z.rows // 2, LANES)) < z.block

    def fine_block(f, carry):
        at = z.block_place(blocks_ref[f]) + 1
        grad = jnp.concatenate(
            [fine_ref[t, pl.ds(f, z.rows, stride=pitch), :] for t in range(z.ct)], axis=1
        )
        hi, lo = hi_lo(grad)
        out = lax.dot_general(
            jnp.concatenate([hi, lo], axis=0),
            w_ref[f],
            dims,
            preferred_element_type=jnp.float32,
        )
        out = out[: z.rows] + out[z.rows :]
        upper, lower = out[: z.rows // 2], out[z.rows // 2 :]
        out = jnp.where(first_half, upper, lower)
        out = out + rolled(jnp.where(first_half, lower, upper), z.block)
        other[at] += out.reshape(z.hg, SUB, LANES)
        return carry

    lax.fori_loop(0, z.fine, fine_block, 0, unroll=16)
    swap_blocks(z, other, field, rate_ref)
    clear_edges(z, field)
    clear_edges(z, other)
    grid, _ = sweeps(z, field, other, rate_ref)

    group = lane_ids((SUB, LANES)) // z.cy
    for a in range(z.n_tx):
        for xq in range(z.xq):
            turned = []
            for q in range(z.nq):
                x = a * z.cx + q * z.xq + xq
                inverse = 1.0 / rate_ref[x]
                turned.append([rolled(grid[x + 1, r] * inverse, q * z.cy) for r in range(z.hg)])
            for b in range(z.n_ty):
                for h in range(z.halves):
                    for r in range(z.hg):
                        total = turned[-(h * z.n_ty + b) % z.nq][r]
                        for j in range(1, z.nq):
                            v = turned[(j - h * z.n_ty - b) % z.nq][r]
                            total = jnp.where(group == j, v, total)
                        every[a * z.n_ty + b, xq * z.rg + h * z.hg + r] = total
    for s in range(z.chips):
        keep_ref[s] = every[z.tile_at(s, False, False)]
        send_ref[s] = every[z.tile_at(s, False, True)]


def finish_kernel(z, alpha_ref, *refs):
    out_ref = refs[-1]
    total = refs[0][...]
    for ref in refs[1:-1]:
        total = total + ref[...]
    b = lax.axis_index("ty")
    for xq in range(z.xq):
        for g in range(z.rg):
            v = total[xq * z.rg + g]
            for q in range(z.nq):
                turn = lax.rem(2 * LANES - (q + g // z.hg * z.n_ty + b) * z.cy, LANES)
                rows = slice(g * SUB, (g + 1) * SUB)
                x = q * z.xq + xq
                out_ref[rows, x, :] = alpha_ref[rows, x, :] + pltpu.roll(v, turn, 1)[:, : z.cy]


def on_device(
    alpha,
    filter_rate,
    block_list,
    interp_weights,
    perturbations,
    obs_cells,
    obs_count,
    departures,
    obs_weight,
):
    z = Sizes(alpha, interp_weights, perturbations, obs_cells, departures)
    f32, bf16 = jnp.float32, jnp.bfloat16
    shape = jax.ShapeDtypeStruct
    coarse = alpha.reshape(z.rows, z.cx, z.cy)
    wanted = block_list.reshape(z.fine)
    weights = interp_weights.reshape(z.fine, z.block, z.bcells)
    cells = obs_cells.reshape(1, z.obs)
    dep = departures.reshape(z.slab_dev, z.obs)
    ow = obs_weight.reshape(z.slab_dev, z.obs)
    axes = ("tx", "ty")
    tile_shape = (z.t_rows, SUB, LANES)
    full_shape = (z.t_rows + 1, SUB, LANES)
    grid_shape = (z.nx + 2, z.hg, SUB, LANES)

    own = pl.pallas_call(
        functools.partial(pack_kernel, z),
        out_shape=shape(full_shape, f32),
        in_specs=[HB, HB],
        out_specs=VM,
        scratch_shapes=[
            pltpu.VMEM(coarse.shape, f32),
            pltpu.VMEM(filter_rate.shape, f32),
            pltpu.SemaphoreType.DMA((2,)),
        ],
        compiler_params=params(8),
        name="pack",
    )(in_hbm(coarse), in_hbm(filter_rate))
    tiles = [own]
    for s in range(1, z.chips):
        tiles.append(lax.ppermute(own, axes, z.chip_perm(s)))
    for s in range(z.chips):
        tiles.append(lax.ppermute(tiles[s], axes, z.core_perm()))

    stacked, column, used = pl.pallas_call(
        functools.partial(prep_kernel, z),
        out_shape=(
            shape((z.fine, 2 * z.block, z.bcells), bf16),
            shape((z.bcells, z.obs), bf16),
            shape((1, z.obs), f32),
        ),
        in_specs=[HB, HB, SM],
        out_specs=(VM, VM, VM),
        scratch_shapes=[
            pltpu.VMEM(weights.shape, f32),
            pltpu.VMEM(cells.shape, jnp.int32),
            pltpu.SemaphoreType.DMA((PREP_CHUNKS + 1,)),
        ],
        compiler_params=params(16),
        cost_estimate=pl.CostEstimate(flops=4_000_000, bytes_accessed=5_000_000, transcendentals=0),
        name="prep",
    )(in_hbm(weights), in_hbm(cells), obs_count)

    pitch = z.rows + PITCH_PAD
    slab_shape = (z.slab_dev, z.fine, z.bcells)
    outs = pl.pallas_call(
        functools.partial(forward_kernel, z),
        out_shape=(
            shape((z.slabs, z.obs + LANES), f32),
            shape((z.nx, SUB, LANES), f32),
            *[shape(slab_shape, f32)] * z.n_mem,
        ),
        in_specs=[SM] + [VM] * (z.tiles + 6),
        out_specs=(VM,) * (2 + z.n_mem),
        scratch_shapes=[
            pltpu.VMEM((z.tiles, *full_shape), f32),
            pltpu.VMEM(grid_shape, f32),
            pltpu.VMEM(grid_shape, f32),
            pltpu.VMEM((z.ct, z.fine * pitch, LANES), f32),
            pltpu.VMEM((z.slabs, z.fine, z.bcells), f32),
        ],
        compiler_params=params(24),
        cost_estimate=pl.CostEstimate(flops=20_000_000, bytes_accessed=8_000_000, transcendentals=0),
        name="forward",
    )(wanted, *tiles, stacked, perturbations, cells, column, dep, ow)
    seen, rate, incs = outs[0], outs[1], outs[2:]

    def ring(step):
        return [(i, (i + step) % z.n_mem) for i in range(z.n_mem)]

    steps = range(1, z.n_mem)
    seens, parts = [seen], []
    for s in steps:
        seens.append(lax.ppermute(seen, "mem", ring(s)))
    for s in steps:
        parts.append(lax.ppermute(incs[s], "mem", ring(s)))

    pitch = z.fine + PITCH_PAD
    weighted, keep, send = pl.pallas_call(
        functools.partial(adjoint_kernel, z),
        out_shape=(
            shape((z.slab_dev, z.obs), f32),
            shape((z.chips, *tile_shape), f32),
            shape((z.chips, *tile_shape), f32),
        ),
        in_specs=[SM] + [VM] * (z.n_mem + 6),
        out_specs=(VM, VM, VM),
        scratch_shapes=[
            pltpu.VMEM((z.tiles, *tile_shape), f32),
            pltpu.VMEM(grid_shape, f32),
            pltpu.VMEM(grid_shape, f32),
            pltpu.VMEM((z.ct, z.rows * pitch, LANES), f32),
            pltpu.VMEM((z.slabs, z.fine, z.bcells), f32),
            pltpu.VMEM((z.n_mem, z.slabs, LANES), f32),
        ],
        compiler_params=params(24),
        cost_estimate=pl.CostEstimate(flops=20_000_000, bytes_accessed=8_000_000, transcendentals=0),
        name="adjoint",
    )(wanted, used, *seens, stacked, perturbations, cells, column, rate)

    came = lax.ppermute(send, axes, z.core_perm())
    sums = [keep[s] + came[s] for s in range(z.chips)]
    sums = [sums[0]] + [lax.ppermute(sums[s], axes, z.chip_perm(s)) for s in range(1, z.chips)]
    gradient = pl.pallas_call(
        functools.partial(finish_kernel, z),
        out_shape=shape((z.rows, z.cx, z.cy), f32),
        in_specs=[VM] * (1 + z.chips),
        out_specs=VM,
        compiler_params=params(8),
        name="finish",
    )(coarse, *sums)
    increment = incs[0]
    for part in parts:
        increment = increment + part
    return (increment, weighted.reshape(departures.shape), gradient.reshape(alpha.shape))


def solution(mesh):
    return jax.shard_map(
        on_device,
        mesh=mesh,
        in_specs=(
            P("mem", None, "tx", "ty"),
            P("tx", "ty"),
            P("tx", "ty", None),
            P("tx", "ty", None, None, None),
            P("mem", None, None, ("tx", "ty"), None),
            P("tx", "ty", None),
            P("tx", "ty"),
            P("tx", "ty", "mem", None),
            P("tx", "ty", "mem", None),
        ),
        out_specs=(
            P("mem", ("tx", "ty"), None),
            P("tx", "ty", "mem", None),
            P("mem", None, "tx", "ty"),
        ),
        check_vma=False,
    )
```

```python
import functools

import jax
import jax.numpy as jnp
from jax import lax
from jax.experimental import pallas as pl
from jax.experimental.pallas import tpu as pltpu
from jax.sharding import PartitionSpec as P


CB = 8
SWEEPS = 4
LANES = 128
SUB = 8
PITCH_PAD = 1
PREP_CHUNKS = 4
SWAP_UNROLL = 16
PRODUCTS = 2


VM = pl.BlockSpec(memory_space=pltpu.VMEM)
HB = pl.BlockSpec(memory_space=pltpu.HBM)
SM = pl.BlockSpec(memory_space=pltpu.SMEM)


def in_hbm(v):
    return pltpu.with_memory_space_constraint(v, pltpu.HBM)


def params(mib):
    return pltpu.CompilerParams(vmem_limit_bytes=mib << 20)


def split2(v, n):
    if n & (n - 1) == 0:
        return v >> (n.bit_length() - 1), v & (n - 1)
    return lax.div(v, n), lax.rem(v, n)


def hi_lo(v):
    hi = v.astype(jnp.bfloat16)
    return hi, (v - hi.astype(jnp.float32)).astype(jnp.bfloat16)


def lane_ids(shape):
    return lax.broadcasted_iota(jnp.int32, shape, len(shape) - 1)


class Sizes:
    def __init__(self, alpha, weights, perts, cells, departures):
        self.n_tx, self.n_ty, self.n_mem = (lax.axis_size(a) for a in ("tx", "ty", "mem"))
        self.tiles = self.n_tx * self.n_ty
        self.chips = self.tiles // 2
        self.members, self.levels, self.cx, self.cy = alpha.shape
        self.rows = self.members * self.levels
        self.rg = self.rows // SUB
        self.fine, self.block, self.bcells = weights.shape[2:]
        self.vars = perts.shape[2]
        self.slabs = self.levels * self.vars
        self.slab_dev = departures.shape[2]
        self.obs = cells.shape[-1]
        self.nx, self.ny = self.n_tx * self.cx, self.n_ty * self.cy
        self.halves = LANES // self.ny
        self.hg = self.rg // self.halves
        self.nq = LANES // self.cy
        self.xq = self.cx // self.nq
        self.t_rows = self.xq * self.rg
        self.ct = self.bcells // LANES
        self.ot = self.obs // LANES
        self.blk_x, self.blk_y = self.cx // CB, self.cy // CB
        assert self.n_tx % 2 == 0 and self.halves * self.ny == LANES and self.ny == CB * CB
        assert self.nq * self.cy == LANES and self.xq * self.nq == self.cx and self.xq <= SUB
        assert self.halves == 2 and self.hg * 2 * SUB == self.rows
        assert self.nq == self.halves * self.n_ty
        assert self.slab_dev * self.ot <= self.slabs

    def block_place(self, bid):
        tile, kb = split2(bid, self.blk_x * self.blk_y)
        a, b = split2(tile, self.n_ty)
        bx, by = split2(kb, self.blk_y)
        return (a * self.blk_x + bx) * CB + b * self.blk_y + by

    def tile_at(self, step, back, other_core):
        tx, ty = lax.axis_index("tx"), lax.axis_index("ty")
        half = self.n_tx // 2
        chip_y, core = split2(tx, 2)
        dy, dx = divmod(step, self.n_ty)
        if back:
            dy, dx = half - dy, self.n_ty - dx
        y = lax.rem(chip_y + dy, half)
        x = lax.rem(ty + dx, self.n_ty)
        if other_core:
            core = 1 - core
        return (y * 2 + core) * self.n_ty + x

    def chip_perm(self, step):
        half = self.n_tx // 2
        dy, dx = divmod(step, self.n_ty)
        pairs = []
        for y in range(half):
            for core in range(2):
                for x in range(self.n_ty):
                    to = ((y + dy) % half * 2 + core) * self.n_ty + (x + dx) % self.n_ty
                    pairs.append(((y * 2 + core) * self.n_ty + x, to))
        return pairs

    def core_perm(self):
        return [(i, (i // self.n_ty ^ 1) * self.n_ty + i % self.n_ty) for i in range(self.tiles)]


def rolled(v, shift):
    shift %= LANES
    return v if shift == 0 else pltpu.roll(v, shift, v.ndim - 1)


def pack_kernel(z, alpha_hbm, rate_hbm, out_ref, alpha_ref, rate_ref, sems):
    copies = [
        pltpu.make_async_copy(alpha_hbm, alpha_ref, sems.at[0]),
        pltpu.make_async_copy(rate_hbm, rate_ref, sems.at[1]),
    ]
    for copy in copies:
        copy.start()
    for copy in copies:
        copy.wait()
    rate_rows, tiles = [], []
    for xq in range(z.xq):
        parts = [alpha_ref[:, q * z.xq + xq, :] for q in range(z.nq)]
        tiles.append(jnp.concatenate(parts, axis=1).reshape(z.rg, SUB, LANES))
        parts = [rate_ref[q * z.xq + xq : q * z.xq + xq + 1, :] for q in range(z.nq)]
        rate_rows.append(jnp.concatenate(parts, axis=1))
    b = lax.axis_index("ty")
    for xq in range(z.xq):
        for g in range(z.rg):
            turn = (g // z.hg * z.n_ty + b) * z.cy
            out_ref[xq * z.rg + g] = pltpu.roll(tiles[xq][g], turn, 1)
    rate_rows += [jnp.zeros((SUB - z.xq, LANES), jnp.float32)]
    out_ref[z.t_rows] = pltpu.roll(jnp.concatenate(rate_rows, axis=0), b * z.cy, 1)


def prep_kernel(z, *refs):
    weights_hbm, cells_hbm, count_ref, stacked_ref, column_ref, used_ref = refs[:6]
    weights_ref, cells_ref, sems = refs[6:]
    k = z.block
    chunk = z.fine // PREP_CHUNKS
    copies = []
    for i in range(PREP_CHUNKS):
        part = pl.ds(i * chunk, chunk)
        copies.append(
            pltpu.make_async_copy(weights_hbm.at[part], weights_ref.at[part], sems.at[i])
        )
    cells_copy = pltpu.make_async_copy(cells_hbm, cells_ref, sems.at[PREP_CHUNKS])
    for copy in [cells_copy] + copies:
        copy.start()
    used_ref[...] = jnp.where(lane_ids((1, z.obs)) < count_ref[0, 0], 1.0, 0.0)
    cells_copy.wait()
    _, col = split2(cells_ref[...], z.bcells)
    ids = lax.broadcasted_iota(jnp.int32, (z.bcells, z.obs), 0)
    column_ref[...] = jnp.where(ids == col, 1.0, 0.0).astype(jnp.bfloat16)

    def one(f, carry):
        hi, lo = hi_lo(weights_ref[f])
        stacked_ref[f, 0:k, :] = hi
        stacked_ref[f, k : 2 * k, :] = lo
        return carry

    for i in range(PREP_CHUNKS):
        copies[i].wait()
        lax.fori_loop(i * chunk, (i + 1) * chunk, one, 0, unroll=2)


def clear_edges(z, ref):
    for x in (0, z.nx + 1):
        ref[x] = jnp.zeros((z.hg, SUB, LANES), jnp.float32)


def sweeps(z, src, dst, rate_ref):
    lane_y = lane_ids((z.hg, SUB, LANES)) % z.ny
    for _ in range(SWEEPS):

        def row(x, carry, src=src, dst=dst):
            c = src[x + 1]
            west = jnp.where(lane_y > 0, rolled(c, 1), 0.0)
            east = jnp.where(lane_y < z.ny - 1, rolled(c, -1), 0.0)
            near = (src[x] + src[x + 2]) + (west + east)
            dst[x + 1] = c + rate_ref[x] * (near - 4.0 * c)
            return carry

        lax.fori_loop(0, z.nx, row, 0, unroll=True)
        src, dst = dst, src
    return src, dst


def swap_blocks(z, src, dst, rate_ref=None):
    lane = lane_ids((SUB, LANES))
    for bit in (1, 2, 4):
        shift = bit * CB
        low = (lane & shift) == 0

        def one(i, carry, src=src, dst=dst):
            bx, r = split2(i, z.hg)
            for j in range(CB):
                if j & bit == 0:
                    at, to = bx * CB + j, bx * CB + (j | bit)
                    a, b = src[at + 1, r], src[to + 1, r]
                    first = jnp.where(low, a, rolled(b, shift))
                    second = jnp.where(low, rolled(a, -shift), b)
                    if rate_ref is not None and bit == 4:
                        first, second = first * rate_ref[at], second * rate_ref[to]
                    dst[at + 1, r] = first
                    dst[to + 1, r] = second
            return carry

        lax.fori_loop(0, z.nx // CB * z.hg, one, 0, unroll=SWAP_UNROLL)
        src, dst = dst, src
    return src, dst


def forward_kernel(z, *refs):
    blocks_ref = refs[0]
    tile_refs = refs[1 : 1 + z.tiles]
    w_ref, pert_ref, cells_ref, column_ref, dep_ref, ow_ref = refs[1 + z.tiles : 7 + z.tiles]
    outs = refs[7 + z.tiles :]
    seen_ref, rate_ref = outs[:2]
    inc_refs = outs[2 : 2 + z.n_mem]
    every, field, other, fine_ref, inc = outs[2 + z.n_mem :]
    me = lax.axis_index("mem")
    for s in range(z.chips):
        every[z.tile_at(s, True, False)] = tile_refs[s][...]
        every[z.tile_at(s, True, True)] = tile_refs[z.chips + s][...]

    clear_edges(z, field)
    clear_edges(z, other)
    group = lane_ids((SUB, LANES)) // z.cy
    for a in range(z.n_tx):
        for q in range(z.nq):
            picks = [divmod((j - q) % z.nq, z.n_ty) for j in range(z.nq)]
            for xq in range(z.xq):
                for r in range(z.hg):
                    total = None
                    for j, (h, b) in enumerate(picks):
                        v = every[a * z.n_ty + b, xq * z.rg + h * z.hg + r]
                        total = v if total is None else jnp.where(group == j, v, total)
                    field[a * z.cx + q * z.xq + xq + 1, r] = rolled(total, -q * z.cy)
            total = None
            for j, (h, b) in enumerate(picks):
                v = rolled(every[a * z.n_ty + b, z.t_rows], h * z.n_ty * z.cy)
                total = v if total is None else jnp.where(group == j, v, total)
            total = rolled(total, -q * z.cy)
            for xq in range(z.xq):
                rate_ref[a * z.cx + q * z.xq + xq] = jnp.broadcast_to(
                    total[xq : xq + 1], (SUB, LANES)
                )

    src, dst = sweeps(z, field, other, rate_ref)
    blocks, _ = swap_blocks(z, src, dst)

    first_half = lane_ids((z.rows // 2, LANES)) < z.block
    low_lanes = lane_ids((z.rows, LANES)) < z.block
    pitch = z.rows + PITCH_PAD

    def fine_block(f, carry):
        v = blocks[z.block_place(blocks_ref[f]) + 1].reshape(z.rows // 2, LANES)
        turned = rolled(v, z.block)
        v = jnp.concatenate(
            [jnp.where(first_half, v, turned), jnp.where(first_half, turned, v)], axis=0
        )
        hi = v.astype(jnp.bfloat16)
        lo = jnp.where(low_lanes, v - hi.astype(jnp.float32), 0.0).astype(jnp.bfloat16)
        lhs = jnp.concatenate([hi, lo], axis=0)
        out = jnp.dot(lhs, w_ref[f], preferred_element_type=jnp.float32)
        out = out[: z.rows] + out[z.rows :]
        start = f * pitch
        for t in range(z.ct):
            fine_ref[t, pl.ds(start, z.rows), :] = out[:, t * LANES : (t + 1) * LANES]
        return carry

    lax.fori_loop(0, z.fine, fine_block, 0, unroll=16)

    def level(l, carry):
        for t in range(z.ct):
            cols = slice(t * LANES, (t + 1) * LANES)
            fine = [
                fine_ref[t, pl.ds(m * z.levels + l, z.fine, stride=pitch), :]
                for m in range(z.members)
            ]
            for v in range(z.vars):
                total = None
                for m in range(z.members):
                    term = fine[m] * pert_ref[m, l, v, :, cols].astype(jnp.float32)
                    total = term if total is None else total + term
                inc[l * z.vars + v, :, cols] = total
        return carry

    lax.fori_loop(0, z.levels, level, 0, unroll=True)

    where, _ = split2(cells_ref[...], z.bcells)
    ids = lax.broadcasted_iota(jnp.int32, (z.fine, z.obs), 0)
    here = ids == where
    n = z.slabs // PRODUCTS
    for i in range(PRODUCTS):
        hi, lo = hi_lo(inc[i * n : (i + 1) * n].reshape(n * z.fine, z.bcells))
        seen = jnp.dot(
            jnp.concatenate([hi, lo], axis=0), column_ref[...], preferred_element_type=jnp.float32
        )
        for k in range(n):
            part = seen[k * z.fine : (k + 1) * z.fine] + seen[(n + k) * z.fine : (n + k + 1) * z.fine]
            seen_ref[i * n + k : i * n + k + 1, : z.obs] = jnp.sum(
                jnp.where(here, part, 0.0), axis=0, keepdims=True
            )
    seen_ref[:, z.obs :] = jnp.zeros((z.slabs, LANES), jnp.float32)
    for g in range(z.n_mem):
        mine = slice(g * z.slab_dev, (g + 1) * z.slab_dev)
        seen_ref[mine, : z.obs] -= jnp.where(g == me, dep_ref[...], 0.0)
    for j in range(z.slab_dev):
        for t in range(z.ot):
            at = j * z.ot + t
            seen_ref[at : at + 1, z.obs :] = ow_ref[j : j + 1, t * LANES : (t + 1) * LANES]
    for s in range(z.n_mem):
        to = lax.rem(me + s, z.n_mem)
        for j in range(z.slab_dev):
            inc_refs[s][j] = inc[to * z.slab_dev + j]


def adjoint_kernel(z, *refs):
    blocks_ref, used_ref = refs[:2]
    seen_refs = refs[2 : 2 + z.n_mem]
    w_ref, pert_ref, cells_ref, column_ref, rate_ref = refs[2 + z.n_mem : 7 + z.n_mem]
    out_ref, keep_ref, send_ref = refs[7 + z.n_mem : 10 + z.n_mem]
    every, field, other, fine_ref, force, obs_w = refs[10 + z.n_mem :]
    me = lax.axis_index("mem")
    total = None
    for s in range(z.n_mem):
        part = seen_refs[s][:, : z.obs]
        total = part if total is None else total + part
        obs_w[lax.rem(me + (z.n_mem - s), z.n_mem)] = seen_refs[s][:, z.obs :]
    used = used_ref[...] > 0.5
    where, _ = split2(cells_ref[...], z.bcells)
    ids = lax.broadcasted_iota(jnp.int32, (z.fine, z.obs), 0)
    here = ids == where
    rows = []
    for s in range(z.slabs):
        g, j = divmod(s, z.slab_dev)
        w = jnp.concatenate([obs_w[g, j * z.ot + t : j * z.ot + t + 1] for t in range(z.ot)], axis=1)
        rows.append(jnp.where(used, w * total[s : s + 1], 0.0))
    for j in range(z.slab_dev):
        mine = rows[j]
        for g in range(1, z.n_mem):
            mine = jnp.where(g == me, rows[g * z.slab_dev + j], mine)
        out_ref[j : j + 1] = mine
    dims = (((1,), (1,)), ((), ()))
    n = z.slabs // PRODUCTS
    for i in range(PRODUCTS):
        his, los = [], []
        for k in range(n):
            hi, lo = hi_lo(rows[i * n + k])
            his.append(jnp.where(here, hi.astype(jnp.float32), 0.0).astype(jnp.bfloat16))
            los.append(jnp.where(here, lo.astype(jnp.float32), 0.0).astype(jnp.bfloat16))
        part = lax.dot_general(
            jnp.concatenate(his + los, axis=0),
            column_ref[...],
            dims,
            preferred_element_type=jnp.float32,
        )
        part = part[: n * z.fine] + part[n * z.fine :]
        force[i * n : (i + 1) * n] = part.reshape(n, z.fine, z.bcells)

    pitch = z.fine + PITCH_PAD

    def level(l, carry):
        for t in range(z.ct):
            cols = slice(t * LANES, (t + 1) * LANES)
            f = [force[l * z.vars + v, :, cols] for v in range(z.vars)]
            for m in range(z.members):
                grad = None
                for v in range(z.vars):
                    term = f[v] * pert_ref[m, l, v, :, cols].astype(jnp.float32)
                    grad = term if grad is None else grad + term
                start = (m * z.levels + l) * pitch
                fine_ref[t, pl.ds(start, z.fine), :] = grad
        return carry

    lax.fori_loop(0, z.levels, level, 0, unroll=True)
    other[...] = jnp.zeros(other.shape, jnp.float32)
    first_half = lane_ids((z.rows // 2, LANES)) < z.block

    def fine_block(f, carry):
        at = z.block_place(blocks_ref[f]) + 1
        grad = jnp.concatenate(
            [fine_ref[t, pl.ds(f, z.rows, stride=pitch), :] for t in range(z.ct)], axis=1
        )
        hi, lo = hi_lo(grad)
        out = lax.dot_general(
            jnp.concatenate([hi, lo], axis=0),
            w_ref[f],
            dims,
            preferred_element_type=jnp.float32,
        )
        out = out[: z.rows] + out[z.rows :]
        upper, lower = out[: z.rows // 2], out[z.rows // 2 :]
        out = jnp.where(first_half, upper, lower)
        out = out + rolled(jnp.where(first_half, lower, upper), z.block)
        other[at] += out.reshape(z.hg, SUB, LANES)
        return carry

    lax.fori_loop(0, z.fine, fine_block, 0, unroll=16)
    swap_blocks(z, other, field, rate_ref)
    clear_edges(z, field)
    clear_edges(z, other)
    grid, _ = sweeps(z, field, other, rate_ref)

    group = lane_ids((SUB, LANES)) // z.cy
    for a in range(z.n_tx):
        for xq in range(z.xq):
            turned = []
            for q in range(z.nq):
                x = a * z.cx + q * z.xq + xq
                inverse = 1.0 / rate_ref[x]
                turned.append([rolled(grid[x + 1, r] * inverse, q * z.cy) for r in range(z.hg)])
            for b in range(z.n_ty):
                for h in range(z.halves):
                    for r in range(z.hg):
                        total = turned[-(h * z.n_ty + b) % z.nq][r]
                        for j in range(1, z.nq):
                            v = turned[(j - h * z.n_ty - b) % z.nq][r]
                            total = jnp.where(group == j, v, total)
                        every[a * z.n_ty + b, xq * z.rg + h * z.hg + r] = total
    for s in range(z.chips):
        keep_ref[s] = every[z.tile_at(s, False, False)]
        send_ref[s] = every[z.tile_at(s, False, True)]


def finish_kernel(z, alpha_ref, *refs):
    out_ref = refs[-1]
    total = refs[0][...]
    for ref in refs[1:-1]:
        total = total + ref[...]
    b = lax.axis_index("ty")
    for xq in range(z.xq):
        for g in range(z.rg):
            v = total[xq * z.rg + g]
            for q in range(z.nq):
                turn = lax.rem(2 * LANES - (q + g // z.hg * z.n_ty + b) * z.cy, LANES)
                rows = slice(g * SUB, (g + 1) * SUB)
                x = q * z.xq + xq
                out_ref[rows, x, :] = alpha_ref[rows, x, :] + pltpu.roll(v, turn, 1)[:, : z.cy]


def on_device(
    alpha,
    filter_rate,
    block_list,
    interp_weights,
    perturbations,
    obs_cells,
    obs_count,
    departures,
    obs_weight,
):
    z = Sizes(alpha, interp_weights, perturbations, obs_cells, departures)
    f32, bf16 = jnp.float32, jnp.bfloat16
    shape = jax.ShapeDtypeStruct
    coarse = alpha.reshape(z.rows, z.cx, z.cy)
    wanted = block_list.reshape(z.fine)
    weights = interp_weights.reshape(z.fine, z.block, z.bcells)
    cells = obs_cells.reshape(1, z.obs)
    dep = departures.reshape(z.slab_dev, z.obs)
    ow = obs_weight.reshape(z.slab_dev, z.obs)
    axes = ("tx", "ty")
    tile_shape = (z.t_rows, SUB, LANES)
    full_shape = (z.t_rows + 1, SUB, LANES)
    grid_shape = (z.nx + 2, z.hg, SUB, LANES)

    own = pl.pallas_call(
        functools.partial(pack_kernel, z),
        out_shape=shape(full_shape, f32),
        in_specs=[HB, HB],
        out_specs=VM,
        scratch_shapes=[
            pltpu.VMEM(coarse.shape, f32),
            pltpu.VMEM(filter_rate.shape, f32),
            pltpu.SemaphoreType.DMA((2,)),
        ],
        compiler_params=params(8),
        name="pack",
    )(in_hbm(coarse), in_hbm(filter_rate))
    tiles = [own]
    for s in range(1, z.chips):
        tiles.append(lax.ppermute(own, axes, z.chip_perm(s)))
    for s in range(z.chips):
        tiles.append(lax.ppermute(tiles[s], axes, z.core_perm()))

    stacked, column, used = pl.pallas_call(
        functools.partial(prep_kernel, z),
        out_shape=(
            shape((z.fine, 2 * z.block, z.bcells), bf16),
            shape((z.bcells, z.obs), bf16),
            shape((1, z.obs), f32),
        ),
        in_specs=[HB, HB, SM],
        out_specs=(VM, VM, VM),
        scratch_shapes=[
            pltpu.VMEM(weights.shape, f32),
            pltpu.VMEM(cells.shape, jnp.int32),
            pltpu.SemaphoreType.DMA((PREP_CHUNKS + 1,)),
        ],
        compiler_params=params(16),
        cost_estimate=pl.CostEstimate(flops=4_000_000, bytes_accessed=5_000_000, transcendentals=0),
        name="prep",
    )(in_hbm(weights), in_hbm(cells), obs_count)

    pitch = z.rows + PITCH_PAD
    slab_shape = (z.slab_dev, z.fine, z.bcells)
    outs = pl.pallas_call(
        functools.partial(forward_kernel, z),
        out_shape=(
            shape((z.slabs, z.obs + LANES), f32),
            shape((z.nx, SUB, LANES), f32),
            *[shape(slab_shape, f32)] * z.n_mem,
        ),
        in_specs=[SM] + [VM] * (z.tiles + 6),
        out_specs=(VM,) * (2 + z.n_mem),
        scratch_shapes=[
            pltpu.VMEM((z.tiles, *full_shape), f32),
            pltpu.VMEM(grid_shape, f32),
            pltpu.VMEM(grid_shape, f32),
            pltpu.VMEM((z.ct, z.fine * pitch, LANES), f32),
            pltpu.VMEM((z.slabs, z.fine, z.bcells), f32),
        ],
        compiler_params=params(24),
        cost_estimate=pl.CostEstimate(flops=20_000_000, bytes_accessed=8_000_000, transcendentals=0),
        name="forward",
    )(wanted, *tiles, stacked, perturbations, cells, column, dep, ow)
    seen, rate, incs = outs[0], outs[1], outs[2:]

    def ring(step):
        return [(i, (i + step) % z.n_mem) for i in range(z.n_mem)]

    steps = range(1, z.n_mem)
    seens, parts = [seen], []
    for s in steps:
        seens.append(lax.ppermute(seen, "mem", ring(s)))
    for s in steps:
        parts.append(lax.ppermute(incs[s], "mem", ring(s)))

    pitch = z.fine + PITCH_PAD
    weighted, keep, send = pl.pallas_call(
        functools.partial(adjoint_kernel, z),
        out_shape=(
            shape((z.slab_dev, z.obs), f32),
            shape((z.chips, *tile_shape), f32),
            shape((z.chips, *tile_shape), f32),
        ),
        in_specs=[SM] + [VM] * (z.n_mem + 6),
        out_specs=(VM, VM, VM),
        scratch_shapes=[
            pltpu.VMEM((z.tiles, *tile_shape), f32),
            pltpu.VMEM(grid_shape, f32),
            pltpu.VMEM(grid_shape, f32),
            pltpu.VMEM((z.ct, z.rows * pitch, LANES), f32),
            pltpu.VMEM((z.slabs, z.fine, z.bcells), f32),
            pltpu.VMEM((z.n_mem, z.slabs, LANES), f32),
        ],
        compiler_params=params(24),
        cost_estimate=pl.CostEstimate(flops=20_000_000, bytes_accessed=8_000_000, transcendentals=0),
        name="adjoint",
    )(wanted, used, *seens, stacked, perturbations, cells, column, rate)

    came = lax.ppermute(send, axes, z.core_perm())
    sums = [keep[s] + came[s] for s in range(z.chips)]
    sums = [sums[0]] + [lax.ppermute(sums[s], axes, z.chip_perm(s)) for s in range(1, z.chips)]
    gradient = pl.pallas_call(
        functools.partial(finish_kernel, z),
        out_shape=shape((z.rows, z.cx, z.cy), f32),
        in_specs=[VM] * (1 + z.chips),
        out_specs=VM,
        compiler_params=params(8),
        name="finish",
    )(coarse, *sums)
    increment = incs[0]
    for part in parts:
        increment = increment + part
    return (increment, weighted.reshape(departures.shape), gradient.reshape(alpha.shape))


def solution(mesh):
    return jax.shard_map(
        on_device,
        mesh=mesh,
        in_specs=(
            P("mem", None, "tx", "ty"),
            P("tx", "ty"),
            P("tx", "ty", None),
            P("tx", "ty", None, None, None),
            P("mem", None, None, ("tx", "ty"), None),
            P("tx", "ty", None),
            P("tx", "ty"),
            P("tx", "ty", "mem", None),
            P("tx", "ty", "mem", None),
        ),
        out_specs=(
            P("mem", ("tx", "ty"), None),
            P("tx", "ty", "mem", None),
            P("mem", None, "tx", "ty"),
        ),
        check_vma=False,
    )
```
